32 devices in a mesh: seq: 4 (over y, x), seg: 4 (over z), head: 2 (over core).
Axes of the slice: x: 2, y: 2, z: 4, core: 2. Of those that a mesh axis runs over, the one named last changes fastest.
Arguments:
- queries: bfloat16 [8, 16384, 128], P('head', ('seg', 'seq')), may hold values from -6 to 6
- keys: bfloat16 [8, 16384, 128], P('head', ('seg', 'seq')), may hold values from -6 to 6
- values: bfloat16 [8, 16384, 128], P('head', ('seg', 'seq')), may hold values from -8 to 8
- teacher: bfloat16 [8, 16384, 128], P('head', ('seg', 'seq')), may hold values from -6 to 6
- query_proj: float32 [128, 16], replicated, may hold values from -0.5 to 0.5
- key_proj: float32 [128, 16], replicated, may hold values from -0.5 to 0.5
Outputs:
- student: bfloat16 [8, 16384, 128], P('head', ('seg', 'seq'))
- query_grad: float32 [128, 16], replicated
- key_grad: float32 [128, 16], replicated
The draws below stay inside these ranges and needn't reach their ends.
All inputs are finite; a program needn't handle non-finite values.
Results may differ from the reference program's by a relative error of at most 0.0014.
The reference program's roundings to bfloat16 on the way count: a program that leaves them out, or rounds other values in their place, can miss the bound.
Values sent between devices are 32-bit elements; how exact they have to be, the bound alone decides.
No kernel may reach another device: no remote copies, remote signals or barrier semaphores. Data moves between devices by JAX's collectives and lax.ppermute only.
A program may use at most 64 MiB of HBM per device.

```python
import math
import jax
import jax.numpy as jnp
import numpy as np
from jax import lax

HD = 128
HEADS = 8
PROJ = 16
TOK_DEV = 1024
TOKENS = 16384
N_SEQ = 4
N_SEG = 4


def draw_values(key, part):
    run_length = TOK_DEV // 4
    runs = TOKENS // run_length
    key_base, key_runs, key_noise = jax.random.split(jax.random.fold_in(key, 17), 3)
    base = jax.random.normal(key_base, (HEADS, 1, 1, HD), jnp.float32)
    run_means = jax.random.normal(key_runs, (HEADS, runs, 1, HD), jnp.float32)
    noise = 0.5 * jax.random.normal(key_noise, (HEADS, runs, run_length, HD), jnp.float32)
    vals = jnp.clip(base + run_means + noise, -8.0, 8.0)
    return vals.reshape(HEADS, TOKENS, HD).astype(jnp.bfloat16)


def block_levels(stream_key, dims, cuts, low, largest):
    loudness = 1.0
    for position, blocks in cuts:
        heights = jax.random.uniform(jax.random.fold_in(jax.random.fold_in(stream_key, 6), position), (blocks,), jnp.float32, low / len(cuts), largest / len(cuts))
        loudness = loudness * jnp.repeat(jnp.exp(heights), dims[position] // blocks).reshape((-1,) + (1,) * (len(dims) - 1 - position))
    return loudness


def normal_values(key, shape, deviation, reach, cuts=(), kind=jnp.bfloat16):
    drawn = deviation * jax.random.normal(key, shape, jnp.float32)
    if cuts:
        drawn = drawn * block_levels(key, shape, cuts, -0.22, 0.18)
    return jnp.clip(drawn, -reach, reach).astype(kind)


def setup_inputs(seed: int = 0) -> dict:
    streams_of = jax.random.split(jax.random.key(seed), 7)
    queries = normal_values(streams_of[0], (HEADS, TOKENS, HD), 1.0, 6.0, ((0, 2), (1, 16)))
    keys = normal_values(streams_of[1], (HEADS, TOKENS, HD), 1.0, 6.0, ((0, 2), (1, 16)))
    values = draw_values(jax.random.fold_in(streams_of[6], 71), 0)
    teacher = normal_values(streams_of[3], (HEADS, TOKENS, HD), 1.0, 6.0, ((0, 2), (1, 16)))
    query_proj = normal_values(streams_of[4], (HD, PROJ), HD ** -0.5, 0.5, (), jnp.float32)
    key_proj = normal_values(streams_of[5], (HD, PROJ), HD ** -0.5, 0.5, (), jnp.float32)
    return dict(queries=queries, keys=keys, values=values, teacher=teacher, query_proj=query_proj, key_proj=key_proj)


highest = lax.Precision.HIGHEST

def feature_tables(width):
    first, second = np.triu_indices(width)
    eye = np.eye(width)
    coef = np.where(first == second, 0.5 ** 0.5, 1.0)
    return (jnp.asarray(eye[first], jnp.float32), jnp.asarray(eye[second], jnp.float32), jnp.asarray(coef, jnp.float32))

def features(proj_t, tables):
    sel_a, sel_b, coef = tables
    left = jnp.dot(sel_a, proj_t, precision=highest)
    right = jnp.dot(sel_b, proj_t, precision=highest)
    return jnp.concatenate([jnp.ones_like(proj_t[:1]), proj_t, coef[:, None] * left * right], 0)

def feature_grad(proj_t, grad_phi, tables):
    sel_a, sel_b, coef = tables
    width = proj_t.shape[0]
    left = jnp.dot(sel_a, proj_t, precision=highest)
    right = jnp.dot(sel_b, proj_t, precision=highest)
    quad = grad_phi[1 + width:] * coef[:, None]
    return grad_phi[1:1 + width] + jnp.dot(sel_a.T, quad * right, precision=highest) + jnp.dot(sel_b.T, quad * left, precision=highest)

def project(weight_b, rows):
    return lax.dot_general(weight_b, rows, (((0,), (1,)), ((), ())), preferred_element_type=jnp.float32)

def head_state(q_h, k_h, v_h, wq_b, wk_b, tables):
    q_t = project(wq_b, q_h)
    k_t = project(wk_b, k_h)
    phi_k = features(k_t, tables)
    state = jnp.dot(phi_k.astype(jnp.bfloat16), v_h, preferred_element_type=jnp.float32)
    return (q_t, k_t, state, lax.optimization_barrier(jnp.sum(phi_k, 1)))

def head_forward(q_t, k_t, v_h, teacher_h, s_prev, z_prev, scale, tables):
    phi_q = features(q_t, tables)
    length = q_t.shape[1]
    scores = lax.dot_general(q_t, k_t, (((0,), (0,)), ((), ())), precision=highest)
    causal = jnp.arange(length)[:, None] >= jnp.arange(length)[None, :]
    weights = jnp.where(causal, 1.0 + scores + 0.5 * scores * scores, 0.0)
    numer = jnp.dot(weights.astype(jnp.bfloat16), v_h, preferred_element_type=jnp.float32)
    numer = numer + lax.dot_general(phi_q, s_prev, (((0,), (0,)), ((), ())), precision=highest)
    denom = lax.optimization_barrier(jnp.sum(weights, 1)) + jnp.dot(z_prev, phi_q, precision=highest)
    student = numer / denom[:, None]
    g_out = scale * (student - teacher_h.astype(jnp.float32))
    g_numer = g_out / denom[:, None]
    g_denom = -lax.optimization_barrier(jnp.sum(g_out * student, 1)) / denom
    g_weights = lax.dot_general(g_numer.astype(jnp.bfloat16), v_h, (((1,), (1,)), ((), ())), preferred_element_type=jnp.float32) + g_denom[:, None]
    g_scores = jnp.where(causal, g_weights * (1.0 + scores), 0.0)
    g_q = lax.dot_general(k_t, g_scores, (((1,), (1,)), ((), ())), precision=highest)
    g_k = jnp.dot(q_t, g_scores, precision=highest)
    g_phi_q = lax.dot_general(s_prev, g_numer, (((1,), (1,)), ((), ())), precision=highest) + z_prev[:, None] * g_denom[None, :]
    g_q = g_q + feature_grad(q_t, g_phi_q, tables)
    g_state = jnp.dot(phi_q, g_numer, precision=highest)
    h_state = jnp.dot(phi_q, g_denom, precision=highest)
    return (student, g_q, g_k, g_state, h_state)

def head_grads(q_h, k_h, v_h, k_t, g_q, g_k, g_next, h_next, tables):
    g_phi_k = lax.dot_general(g_next.astype(jnp.bfloat16), v_h, (((1,), (1,)), ((), ())), preferred_element_type=jnp.float32) + h_next[:, None]
    g_k = g_k + feature_grad(k_t, g_phi_k, tables)
    grad_q = lax.dot_general(q_h, g_q.astype(jnp.bfloat16), (((0,), (1,)), ((), ())), preferred_element_type=jnp.float32)
    grad_k = lax.dot_general(k_h, g_k.astype(jnp.bfloat16), (((0,), (1,)), ((), ())), preferred_element_type=jnp.float32)
    return (grad_q, grad_k)

def exclusive(array):
    return jnp.concatenate([jnp.zeros_like(array[:1]), jnp.cumsum(array, 0)[:-1]], 0)

def reference(queries, keys, values, teacher, query_proj, key_proj):
    tables = feature_tables(PROJ)
    wq_b = query_proj.astype(jnp.bfloat16)
    wk_b = key_proj.astype(jnp.bfloat16)
    blocks_all = N_SEQ * N_SEG
    scale = 1.0 / math.sqrt(HEADS * TOKENS)

    def block(array, index):
        return lax.dynamic_slice_in_dim(array, index * TOK_DEV, TOK_DEV, 1)

    def group_state(index):
        outs = lax.map(lambda xs: head_state(xs[0], xs[1], xs[2], wq_b, wk_b, tables), (block(queries, index), block(keys, index), block(values, index)))
        return (outs[2], outs[3])
    order = jnp.arange(blocks_all, dtype=jnp.int32)
    states, counts = lax.map(group_state, order)
    s_prev = exclusive(states)
    z_prev = exclusive(counts)

    def group_forward(index):
        q_b, k_b, v_b, t_b = (block(queries, index), block(keys, index), block(values, index), block(teacher, index))
        q_t, k_t, unused_a, unused_b = lax.map(lambda xs: head_state(xs[0], xs[1], xs[2], wq_b, wk_b, tables), (q_b, k_b, v_b))
        student, g_q, g_k, g_state, h_state = lax.map(lambda xs: head_forward(xs[0], xs[1], xs[2], xs[3], xs[4], xs[5], scale, tables), (q_t, k_t, v_b, t_b, s_prev[index], z_prev[index]))
        return (student.astype(jnp.bfloat16), g_q, g_k, g_state, h_state)
    students, g_qs, g_ks, g_states, h_states = lax.map(group_forward, order)
    g_next = jnp.flip(exclusive(jnp.flip(g_states, 0)), 0)
    h_next = jnp.flip(exclusive(jnp.flip(h_states, 0)), 0)

    def group_grads(index):
        q_b, k_b, v_b = (block(queries, index), block(keys, index), block(values, index))
        k_t = lax.map(lambda xs: project(wk_b, xs), k_b)
        grad_q, grad_k = lax.map(lambda xs: head_grads(xs[0], xs[1], xs[2], xs[3], xs[4], xs[5], xs[6], xs[7], tables), (q_b, k_b, v_b, k_t, g_qs[index], g_ks[index], g_next[index], h_next[index]))
        return (lax.optimization_barrier(jnp.sum(grad_q, 0)), lax.optimization_barrier(jnp.sum(grad_k, 0)))
    grad_q, grad_k = lax.map(group_grads, order)
    output = jnp.moveaxis(students, 0, 1).reshape(HEADS, TOKENS, HD)
    return (output, lax.optimization_barrier(jnp.sum(grad_q, 0)), lax.optimization_barrier(jnp.sum(grad_k, 0)))
```

```python
import functools
import math

import jax
import jax.numpy as jnp
import numpy as np
from jax import lax
from jax.experimental import pallas as pl
from jax.experimental.pallas import tpu as pltpu
from jax.sharding import PartitionSpec as P

f32 = jnp.float32
bf16 = jnp.bfloat16
HALF = 0.5**0.5
LANES = 128
NT = (((1,), (1,)), ((), ()))


class Dims:
    def __init__(self, width):
        self.width = width
        self.half = width // 2
        self.quad = width * (width + 1) // 2
        self.lin = self.quad
        self.const = self.quad + width
        self.feats = self.const + 1
        self.lanes = -(-self.feats // LANES) * LANES
        self.count_rows = self.lanes // LANES
        self.rows = -(-(self.feats + self.count_rows) // 8) * 8


def selections(dm):
    w = dm.width
    first = np.concatenate([np.tile(np.arange(w), dm.half), np.arange(dm.half)])
    shift = np.concatenate([np.repeat(np.arange(dm.half), w), np.full(dm.half, dm.half)])
    second = (first + shift) % w
    sel_a = np.zeros((w, dm.lanes), np.float32)
    sel_b = np.zeros((w, dm.lanes), np.float32)
    sel_a[first, np.arange(dm.quad)] = 1.0
    sel_b[second, np.arange(dm.quad)] = 1.0
    sel_a[np.arange(w), dm.lin + np.arange(w)] = 1.0
    table = np.zeros((8, dm.lanes), np.float32)
    table[0, dm.const] = 1.0
    table[1, dm.lin : dm.feats] = 1.0
    table[2, : dm.feats] = 1.0
    table[2, :w] = HALF
    rep = np.tile(np.eye(w, dtype=np.float32), (1, LANES // w))
    as_b = lambda a: jnp.asarray(a, bf16)
    return as_b(sel_a), as_b(sel_b), as_b(sel_b[:, : dm.quad].T), as_b(rep), jnp.asarray(table)


def dot(a, b, dims=(((1,), (0,)), ((), ()))):
    return lax.dot_general(a, b, dims, preferred_element_type=f32)


def split2(x):
    hi = x.astype(bf16)
    return hi, (x - hi.astype(f32)).astype(bf16)


def split3(x):
    hi = x.astype(bf16)
    rest = x - hi.astype(f32)
    mid = rest.astype(bf16)
    return hi, mid, (rest - mid.astype(f32)).astype(bf16)


def rolled(weight, sel_t):
    return dot(sel_t, weight, NT).astype(bf16)


def features_t(ext, dm):
    w = dm.width
    base = ext[:w]
    parts = [HALF * base * base]
    for d in range(1, dm.half):
        parts.append(ext[d * w : (d + 1) * w] * base)
    parts.append(ext[dm.half * w : dm.quad] * base[: dm.half])
    parts.append(base)
    tail = dm.rows - dm.const
    rows = lax.broadcasted_iota(jnp.int32, (tail, ext.shape[1]), 0)
    parts.append(jnp.where(rows == 0, 1.0, 0.0).astype(f32))
    return jnp.concatenate(parts, 0)


def features_rows(rows, weight, sel_a, sel_b, table):
    left = dot(rows, dot(weight, sel_a).astype(bf16)) + table[0:1]
    right = dot(rows, dot(weight, sel_b).astype(bf16)) + table[1:2]
    return table[2:3] * left * right


def feature_grad_t(ext, g, dm):
    w, half = dm.width, dm.half
    base = ext[:w]
    total = g[dm.lin : dm.lin + w] + (2.0 * HALF) * g[:w] * base
    for d in range(1, half):
        quad = g[d * w : (d + 1) * w]
        total = total + quad * ext[d * w : (d + 1) * w]
        back = quad * base
        total = total + jnp.concatenate([back[w - d :], back[: w - d]], 0)
    quad = g[half * w : dm.quad]
    return total + jnp.concatenate([quad * base[half:], quad * base[:half]], 0)


def with_count(state, count, dm):
    rows = lax.broadcasted_iota(jnp.int32, state.shape, 0)
    for c in range(dm.count_rows):
        state = jnp.where(rows == dm.feats + c, count[:, c * LANES : (c + 1) * LANES], state)
    return state


def count_of(state, dm):
    return jnp.concatenate([state[dm.feats + c : dm.feats + c + 1] for c in range(dm.count_rows)], 1)


def state_kernel(dm, k_ref, v_ref, wk_ref, selt_ref, out_ref):
    wk = wk_ref[...].astype(bf16)
    ext = dot(rolled(wk, selt_ref[...]), k_ref[0], NT)
    phi = features_t(ext, dm)
    state = dot(phi.astype(bf16), v_ref[0])
    part = phi[:, :LANES]
    for c in range(1, phi.shape[1] // LANES):
        part = part + phi[:, c * LANES : (c + 1) * LANES]
    count = lax.dot_general(
        jnp.ones((8, LANES), f32), part, NT, precision=lax.Precision.HIGHEST, preferred_element_type=f32
    )[0:1]
    count = jnp.concatenate([count, jnp.zeros((1, dm.lanes - dm.rows), f32)], 1)
    out_ref[0] = with_count(state, count, dm)


def packs(q, k, wq, wk, rep, selt, dm):
    w = dm.width
    q1, q2, q3 = split3(dot(q, dot(wq, rep).astype(bf16)))
    group = lax.broadcasted_iota(jnp.int32, (1, LANES), 1)
    zero = jnp.zeros((), bf16)

    def at(lo, hi):
        return (group >= lo * w) & (group < hi * w)

    q_pack = jnp.where(at(0, 3), q1, jnp.where(at(3, 5), q2, jnp.where(at(5, 6), q3, zero)))
    q_pack = jnp.where(group == 6 * w, jnp.ones((), bf16), q_pack)
    k_t = dot(rolled(wk, selt[:w]), k, NT)
    k1, k2, k3 = split3(k_t)
    rows = lax.broadcasted_iota(jnp.int32, (LANES - 6 * w, k_t.shape[1]), 0)
    last = jnp.where(rows == 0, 1.0, 0.0).astype(bf16)
    return q_pack, jnp.concatenate([k1, k2, k3, k1, k2, k1, last], 0), k1, k2


def intra_kernel(dm, tile, q_ref, k_ref, v_ref, wq_ref, wk_ref, rep_ref, selt_ref, numer_ref, denom_ref):
    q_pack, k_pack, _, _ = packs(
        q_ref[0], k_ref[0], wq_ref[...].astype(bf16), wk_ref[...].astype(bf16), rep_ref[...], selt_ref[...], dm
    )
    tokens = q_pack.shape[0]
    below = lax.broadcasted_iota(jnp.int32, (tile, tile), 0) >= lax.broadcasted_iota(jnp.int32, (tile, tile), 1)
    for i in range(tokens // tile):
        rows = slice(i * tile, (i + 1) * tile)
        numer = jnp.zeros((tile, v_ref.shape[2]), f32)
        denom = jnp.zeros((tile, LANES), f32)
        for j in range(i + 1):
            cols = slice(j * tile, (j + 1) * tile)
            t = dot(q_pack[rows], k_pack[:, cols])
            weight = (0.5 * t) * t + 0.5
            if j == i:
                weight = jnp.where(below, weight, 0.0)
            for c in range(tile // LANES):
                denom = denom + weight[:, c * LANES : (c + 1) * LANES]
            numer = numer + dot(weight.astype(bf16), v_ref[0, cols, :])
        numer_ref[0, rows, :] = numer
        denom_ref[0, rows, :] = denom


def gather_slots(me_ref, slots, scr):
    me = me_ref[0]
    size = slots[0].shape[0]
    for d, slot in enumerate(slots):
        scr[pl.ds(pl.multiple_of((me ^ d) * size, 8), size), :] = slot[...]


def head_rows(scr, dm):
    return scr[pl.ds(pl.multiple_of(pl.program_id(0) * dm.rows, 8), dm.rows), :]


def forward_kernel(
    dm, scale, n, me_ref, q_ref, wq_ref, sela_ref, selb_ref, selt_ref, table_ref, numer_ref, denom_ref, teacher_ref, *rest
):
    slots, (student_ref, g_ref, gd_ref, back_ref, scr) = rest[:n], rest[n:]

    @pl.when(pl.program_id(0) == 0)
    def _():
        gather_slots(me_ref, slots, scr)

    state = head_rows(scr, dm)
    wq = wq_ref[...].astype(bf16)
    q = q_ref[0]
    table = table_ref[...]
    phi = features_rows(q, wq, sela_ref[...], selb_ref[...], table)
    s1, s2 = split2(state)
    s_pack = jnp.concatenate([s1, s2], 1)
    s_pack = jnp.concatenate([s_pack, jnp.zeros((dm.lanes - dm.rows, s_pack.shape[1]), bf16)], 0)
    p1, p2 = split2(phi)
    prod = dot(p1, s_pack) + dot(p2, s_pack)
    hd = state.shape[1]
    numer = numer_ref[0] + (prod[:, :hd] + prod[:, hd:])
    weighted = phi * count_of(state, dm)
    part = denom_ref[0]
    for c in range(dm.lanes // LANES):
        part = part + weighted[:, c * LANES : (c + 1) * LANES]
    denom = jnp.sum(part, 1, keepdims=True)
    inv = 1.0 / denom
    y = numer * inv
    student_ref[0] = y.astype(bf16)
    g_out = scale * (y - teacher_ref[0].astype(f32))
    g_numer = g_out * inv
    g_denom = -jnp.sum(g_out * y, 1, keepdims=True) * inv
    g_ref[0] = g_numer
    gd_ref[0] = jnp.broadcast_to(g_denom, gd_ref.shape[1:])
    phi_t = features_t(dot(rolled(wq, selt_ref[...]), q, NT), dm)
    t1, t2 = split2(phi_t)
    g1, g2 = split2(g_numer)
    g_pack = jnp.concatenate([g1, g2], 1)
    prod = dot(t1, g_pack) + dot(t2, g_pack)
    back = prod[:, :hd] + prod[:, hd:]
    back_ref[0] = with_count(back, jnp.sum(phi * g_denom, 0, keepdims=True), dm)


def backward_kernel(
    dm, tile, n, me_ref, q_ref, k_ref, v_ref, wq_ref, wk_ref, rep_ref, selt_ref, g_ref, gd_ref, *rest
):
    slots, (gk_ref, wgrad_ref, scr) = rest[:n], rest[n:]

    @pl.when(pl.program_id(0) == 0)
    def _():
        gather_slots(me_ref, slots, scr)
        wgrad_ref[...] = jnp.zeros_like(wgrad_ref)

    state = head_rows(scr, dm)
    wq = wq_ref[...].astype(bf16)
    q = q_ref[0]
    selt = selt_ref[...]
    q_pack, k_pack, k1, k2 = packs(q, k_ref[0], wq, wk_ref[...].astype(bf16), rep_ref[...], selt, dm)
    k_two = jnp.concatenate([k1, k2], 0)
    ext = dot(rolled(wq, selt), q, NT)
    w = dm.width
    q1, q2 = split2(ext[:w])
    q_two = jnp.concatenate([q1, q2], 0)
    g_numer = g_ref[0]
    g_hi = g_numer.astype(bf16)
    tokens = q.shape[0]
    below = lax.broadcasted_iota(jnp.int32, (tile, tile), 0) >= lax.broadcasted_iota(jnp.int32, (tile, tile), 1)
    count = tokens // tile
    g_k = [jnp.zeros((w, tile), f32) for _ in range(count)]
    g_q = []
    for i in range(count):
        rows = slice(i * tile, (i + 1) * tile)
        gd = gd_ref[0, rows, :]
        gd = jnp.concatenate([gd] * (tile // LANES), 1)
        total = jnp.zeros((w, tile), f32)
        for j in range(i + 1):
            cols = slice(j * tile, (j + 1) * tile)
            t = dot(q_pack[rows], k_pack[:, cols])
            score = (dot(g_hi[rows], v_ref[0, cols, :], NT) + gd) * t
            if j == i:
                score = jnp.where(below, score, 0.0)
            hi, lo = split2(score)
            both = dot(k_two[:, cols], hi, NT)
            total = total + (both[:w] + both[w:]) + dot(k1[:, cols], lo, NT)
            both = dot(q_two[:, rows], hi)
            g_k[j] = g_k[j] + (both[:w] + both[w:]) + dot(q1[:, rows], lo)
        g_q.append(total)
    gk_ref[0] = jnp.concatenate(g_k, 1)
    row = lax.broadcasted_iota(jnp.int32, (dm.rows, dm.lanes), 0)
    lane = lax.broadcasted_iota(jnp.int32, (dm.rows, dm.lanes), 1)
    column = jnp.sum(jnp.where(row == lane, count_of(state, dm), 0.0), 1, keepdims=True)
    first = lax.broadcasted_iota(jnp.int32, (1, LANES), 1) == 0
    s_aug = jnp.concatenate([state, jnp.where(first, column, 0.0)], 1)
    g_aug = jnp.concatenate([g_numer, jnp.where(first, gd_ref[0], 0.0)], 1)
    s1, s2 = split2(s_aug)
    a1, a2 = split2(g_aug)
    both = dot(jnp.concatenate([s1, s2], 0), a1, NT)
    g_phi = both[: dm.rows] + both[dm.rows :] + dot(s1, a2, NT)
    total = jnp.concatenate(g_q, 1) + feature_grad_t(ext, g_phi, dm)
    wgrad_ref[...] += dot(total.astype(bf16), q)


def key_kernel(dm, n, me_ref, k_ref, v_ref, wk_ref, selt_ref, gk_ref, *rest):
    slots, (wgrad_ref, scr) = rest[:n], rest[n:]

    @pl.when(pl.program_id(0) == 0)
    def _():
        gather_slots(me_ref, slots, scr)
        wgrad_ref[...] = jnp.zeros_like(wgrad_ref)

    state = head_rows(scr, dm)
    k = k_ref[0]
    ext = dot(rolled(wk_ref[...].astype(bf16), selt_ref[...]), k, NT)
    row = lax.broadcasted_iota(jnp.int32, (dm.rows, dm.lanes), 0)
    lane = lax.broadcasted_iota(jnp.int32, (dm.rows, dm.lanes), 1)
    column = jnp.sum(jnp.where(row == lane, count_of(state, dm), 0.0), 1, keepdims=True)
    g_phi = dot(state.astype(bf16), v_ref[0], NT) + column
    total = gk_ref[0] + feature_grad_t(ext, g_phi, dm)
    wgrad_ref[...] += dot(total.astype(bf16), k)


VMEM_LIMIT = 24 * 1024 * 1024


def head_spec(array):
    return pl.BlockSpec((1,) + array.shape[1:], lambda h: (h, 0, 0))


def whole(array):
    return pl.BlockSpec(array.shape, lambda h: (0,) * array.ndim)


SMEM = pl.BlockSpec(memory_space=pltpu.SMEM)


def call(body, heads, args, specs, outs, out_specs, scratch, flops, name):
    moved = sum(math.prod(a.shape) * a.dtype.itemsize for a in list(args) + list(outs))
    return pl.pallas_call(
        body,
        grid=(heads,),
        in_specs=specs,
        out_specs=out_specs,
        out_shape=outs,
        scratch_shapes=scratch,
        compiler_params=pltpu.CompilerParams(
            dimension_semantics=("arbitrary",), vmem_limit_bytes=VMEM_LIMIT
        ),
        cost_estimate=pl.CostEstimate(flops=flops, bytes_accessed=moved, transcendentals=0),
        name=name,
    )(*args)


def shifted(array, axis, pairs):
    return lax.ppermute(array, axis, pairs)


def carried(local, backward):
    n, me = lax.axis_size("seq"), lax.axis_index("seq")
    size = local.shape[0] // n

    def swap(array, d):
        return array if d == 0 else shifted(array, "seq", [(i, i ^ d) for i in range(n)])

    got = [swap(lax.dynamic_slice_in_dim(local, (me ^ d) * size, size, 0), d) for d in range(n)]
    total = functools.reduce(jnp.add, got)
    before = []
    for d in range(n):
        order = me ^ d
        keep = [((me ^ e) > order) if backward else ((me ^ e) < order) for e in range(n)]
        before.append(functools.reduce(jnp.add, [jnp.where(k, g, 0.0) for k, g in zip(keep, got)]))
    m = lax.axis_size("seg")
    far = None
    for d in range(1, m):
        pairs = [(i, i - d) for i in range(d, m)] if backward else [(i, i + d) for i in range(m - d)]
        piece = shifted(total, "seg", pairs)
        far = piece if far is None else far + piece
    if far is not None:
        before = [b + far for b in before]
    return [swap(b, d) for d, b in enumerate(before)]


def summed(array):
    for axis in ("head", "seq", "seg"):
        n = lax.axis_size(axis)
        got = [shifted(array, axis, [(i, i ^ d) for i in range(n)]) for d in range(1, n)]
        array = functools.reduce(jnp.add, [array] + got)
    return array


def shards(queries, keys, values, teacher, query_proj, key_proj):
    heads, tokens, hd = queries.shape
    dm = Dims(query_proj.shape[1])
    n = lax.axis_size("seq")
    heads_all = heads * lax.axis_size("head")
    tokens_all = tokens * n * lax.axis_size("seg")
    scale = 1.0 / math.sqrt(heads_all * tokens_all)
    tile = min(256, tokens)
    sel_a, sel_b, sel_t, rep, table = selections(dm)
    me = jnp.reshape(lax.axis_index("seq").astype(jnp.int32), (1,))
    state_shape = jax.ShapeDtypeStruct((heads, dm.rows, hd), f32)
    tok_shape = jax.ShapeDtypeStruct((heads, tokens, hd), f32)
    lane_shape = jax.ShapeDtypeStruct((heads, tokens, LANES), f32)
    grad_shape = jax.ShapeDtypeStruct((dm.width, hd), f32)
    gk_shape = jax.ShapeDtypeStruct((heads, dm.width, tokens), f32)
    scratch = [pltpu.VMEM((heads * dm.rows, hd), f32)]
    square = heads * tokens * tokens

    states = call(
        functools.partial(state_kernel, dm),
        heads,
        (keys, values, key_proj, sel_t),
        [head_spec(keys), head_spec(values), whole(key_proj), whole(sel_t)],
        [state_shape],
        [head_spec(state_shape)],
        [],
        4 * heads * tokens * dm.rows * hd,
        "states",
    )[0]
    numer, denom = call(
        functools.partial(intra_kernel, dm, tile),
        heads,
        (queries, keys, values, query_proj, key_proj, rep, sel_t),
        [head_spec(queries), head_spec(keys), head_spec(values)]
        + [whole(a) for a in (query_proj, key_proj, rep, sel_t)],
        [tok_shape, lane_shape],
        [head_spec(tok_shape), head_spec(lane_shape)],
        [],
        4 * square * hd,
        "intra",
    )
    prev = carried(states.reshape(heads * dm.rows, hd), False)
    student, g_numer, g_denom, back = call(
        functools.partial(forward_kernel, dm, scale, n),
        heads,
        (me, queries, query_proj, sel_a, sel_b, sel_t, table, numer, denom, teacher, *prev),
        [SMEM, head_spec(queries)]
        + [whole(a) for a in (query_proj, sel_a, sel_b, sel_t, table)]
        + [head_spec(numer), head_spec(denom), head_spec(teacher)]
        + [whole(a) for a in prev],
        [jax.ShapeDtypeStruct(tok_shape.shape, bf16), tok_shape, lane_shape, state_shape],
        [head_spec(tok_shape), head_spec(tok_shape), head_spec(lane_shape), head_spec(state_shape)],
        scratch,
        8 * heads * tokens * dm.lanes * hd,
        "forward",
    )
    g_k, q_grad = call(
        functools.partial(backward_kernel, dm, tile, n),
        heads,
        (me, queries, keys, values, query_proj, key_proj, rep, sel_t, g_numer, g_denom, *prev),
        [SMEM, head_spec(queries), head_spec(keys), head_spec(values)]
        + [whole(a) for a in (query_proj, key_proj, rep, sel_t)]
        + [head_spec(g_numer), head_spec(g_denom)]
        + [whole(a) for a in prev],
        [gk_shape, grad_shape],
        [head_spec(gk_shape), whole(grad_shape)],
        scratch,
        8 * square * hd,
        "backward",
    )
    later = carried(back.reshape(heads * dm.rows, hd), True)
    k_grad = call(
        functools.partial(key_kernel, dm, n),
        heads,
        (me, keys, values, key_proj, sel_t, g_k, *later),
        [SMEM, head_spec(keys), head_spec(values), whole(key_proj), whole(sel_t), head_spec(g_k)]
        + [whole(a) for a in later],
        [grad_shape],
        [whole(grad_shape)],
        scratch,
        4 * heads * tokens * dm.rows * hd,
        "keygrad",
    )[0]
    grads = summed(jnp.concatenate([q_grad, k_grad], 0))
    return student, grads[: dm.width].T, grads[dm.width :].T


def solution(mesh):
    in_specs = (
        P("head", ("seg", "seq"), None),
        P("head", ("seg", "seq"), None),
        P("head", ("seg", "seq"), None),
        P("head", ("seg", "seq"), None),
        P(),
        P(),
    )
    out_specs = (P("head", ("seg", "seq"), None), P(), P())
    return jax.shard_map(shards, mesh=mesh, in_specs=in_specs, out_specs=out_specs, check_vma=False)
```

```python
import functools
import math

import jax
import jax.numpy as jnp
from jax import lax
from jax.experimental import pallas as pl
from jax.experimental.pallas import tpu as pltpu
from jax.sharding import PartitionSpec as P

f32 = jnp.float32
bf16 = jnp.bfloat16
HALF = 0.5**0.5
LANES = 128
NT = (((1,), (1,)), ((), ()))


class Dims:
    def __init__(self, width):
        self.width = width
        self.half = width // 2
        self.shift = width.bit_length() - 1
        assert width == 1 << self.shift
        self.quad = width * (width + 1) // 2
        self.lin = self.quad
        self.const = self.quad + width
        self.feats = self.const + 1
        self.lanes = -(-self.feats // LANES) * LANES
        self.count_rows = self.lanes // LANES
        self.rows = -(-(self.feats + self.count_rows) // 8) * 8


def positions(shape, dim):
    return lax.broadcasted_iota(jnp.int32, shape, dim)


def one_hot(hit):
    return jnp.where(hit, 1.0, 0.0).astype(bf16)


def first_of(dm, f):
    return jnp.where(f < dm.quad, f & (dm.width - 1), f - dm.lin)


def second_of(dm, f):
    return (f + (f >> dm.shift)) & (dm.width - 1)


def dot(a, b, dims=(((1,), (0,)), ((), ()))):
    return lax.dot_general(a, b, dims, preferred_element_type=f32)


def split2(x):
    hi = x.astype(bf16)
    return hi, (x - hi.astype(f32)).astype(bf16)


def split3(x):
    hi = x.astype(bf16)
    rest = x - hi.astype(f32)
    mid = rest.astype(bf16)
    return hi, mid, (rest - mid.astype(f32)).astype(bf16)


def rolled(w_t, dm):
    shape = (dm.quad, dm.width)
    return dot(one_hot(second_of(dm, positions(shape, 0)) == positions(shape, 1)), w_t).astype(bf16)


def repeated(w_t, dm):
    shape = (LANES, dm.width)
    return dot(one_hot((positions(shape, 0) & (dm.width - 1)) == positions(shape, 1)), w_t).astype(bf16)


def sides(w_t, dm):
    shape = (dm.lanes, dm.width)
    f, j = positions(shape, 0), positions(shape, 1)
    left = dot(one_hot(first_of(dm, f) == j), w_t).astype(bf16)
    right = dot(one_hot((f < dm.quad) & (second_of(dm, f) == j)), w_t).astype(bf16)
    return left, right


def features_t(ext, dm):
    w = dm.width
    base = ext[:w]
    parts = [HALF * base * base]
    for d in range(1, dm.half):
        parts.append(ext[d * w : (d + 1) * w] * base)
    parts.append(ext[dm.half * w : dm.quad] * base[: dm.half])
    parts.append(base)
    tail = dm.rows - dm.const
    rows = lax.broadcasted_iota(jnp.int32, (tail, ext.shape[1]), 0)
    parts.append(jnp.where(rows == 0, 1.0, 0.0).astype(f32))
    return jnp.concatenate(parts, 0)


def features_rows(rows, w_t, dm):
    left, right = sides(w_t, dm)
    f = positions((1, dm.lanes), 1)
    left = dot(rows, left, NT) + jnp.where(f == dm.const, 1.0, 0.0)
    right = dot(rows, right, NT) + jnp.where((f >= dm.lin) & (f < dm.feats), 1.0, 0.0)
    return jnp.where(f < dm.width, HALF, 1.0) * left * right


def feature_grad_t(ext, g, dm):
    w, half = dm.width, dm.half
    base = ext[:w]
    total = g[dm.lin : dm.lin + w] + (2.0 * HALF) * g[:w] * base
    for d in range(1, half):
        quad = g[d * w : (d + 1) * w]
        total = total + quad * ext[d * w : (d + 1) * w]
        back = quad * base
        total = total + jnp.concatenate([back[w - d :], back[: w - d]], 0)
    quad = g[half * w : dm.quad]
    return total + jnp.concatenate([quad * base[half:], quad * base[:half]], 0)


def with_count(state, count, dm):
    rows = lax.broadcasted_iota(jnp.int32, state.shape, 0)
    for c in range(dm.count_rows):
        state = jnp.where(rows == dm.feats + c, count[:, c * LANES : (c + 1) * LANES], state)
    return state


def count_of(state, dm):
    return jnp.concatenate([state[dm.feats + c : dm.feats + c + 1] for c in range(dm.count_rows)], 1)


def state_kernel(dm, n, me_ref, *rest):
    sources, slots, kept, scr, sems, last = rest[:6], rest[6 : 6 + n], rest[6 + n : 12 + n], *rest[12 + n :]
    k_hbm, v_hbm, q_hbm, t_hbm, wk_hbm, wq_hbm = sources
    k_ref, v_ref, q_ref, t_ref, wk_ref, wq_ref = kept
    heads = k_ref.shape[0]
    first = pltpu.make_async_copy(wk_hbm, wk_ref, last.at[0])
    keys = [pltpu.make_async_copy(k_hbm.at[h], k_ref.at[h], sems.at[h]) for h in range(heads)]
    values = [pltpu.make_async_copy(v_hbm.at[h], v_ref.at[h], sems.at[heads + h]) for h in range(heads)]
    others = [
        pltpu.make_async_copy(wq_hbm, wq_ref, last.at[1]),
        pltpu.make_async_copy(q_hbm, q_ref, last.at[2]),
        pltpu.make_async_copy(t_hbm, t_ref, last.at[3]),
    ]
    first.start()
    for h in range(heads):
        keys[h].start()
        values[h].start()
    for copy in others:
        copy.start()
    first.wait()
    w_ext = rolled(wk_ref[...].astype(bf16), dm)
    for h in range(heads):
        keys[h].wait()
        phi = features_t(dot(w_ext, k_ref[h], NT), dm)
        values[h].wait()
        state = dot(phi.astype(bf16), v_ref[h])
        part = phi[:, :LANES]
        for c in range(1, phi.shape[1] // LANES):
            part = part + phi[:, c * LANES : (c + 1) * LANES]
        count = lax.dot_general(
            jnp.ones((8, LANES), f32), part, NT, precision=lax.Precision.HIGHEST, preferred_element_type=f32
        )[0:1]
        count = jnp.concatenate([count, jnp.zeros((1, dm.lanes - dm.rows), f32)], 1)
        scr[h * dm.rows : (h + 1) * dm.rows, :] = with_count(state, count, dm)
    scatter_slots(me_ref, slots, scr)
    for copy in others:
        copy.wait()


def packs(q, k, wq, wk, dm):
    w = dm.width
    q1, q2, q3 = split3(dot(q, repeated(wq, dm), NT))
    group = positions((1, LANES), 1)
    zero = jnp.zeros((), bf16)

    def at(lo, hi):
        return (group >= lo * w) & (group < hi * w)

    q_pack = jnp.where(at(0, 3), q1, jnp.where(at(3, 5), q2, jnp.where(at(5, 6), q3, zero)))
    q_pack = jnp.where(group == 6 * w, jnp.ones((), bf16), q_pack)
    k_t = dot(wk, k, NT)
    k1, k2, k3 = split3(k_t)
    last = one_hot(positions((LANES - 6 * w, k_t.shape[1]), 0) == 0)
    return q_pack, jnp.concatenate([k1, k2, k3, k1, k2, k1, last], 0), k1, k2


def intra_kernel(dm, tile, h0, q_ref, k_ref, v_ref, wq_ref, wk_ref, numer_ref, denom_ref, phi_ref, phi_t_ref):
    h = pl.program_id(0)
    q, k, v = q_ref[h0 + h], k_ref[h0 + h], v_ref.at[h0 + h]
    wq = wq_ref[...].astype(bf16)
    phi_ref[h] = features_rows(q, wq, dm)
    phi_t_ref[h] = features_t(dot(rolled(wq, dm), q, NT), dm)
    q_pack, k_pack, _, _ = packs(q, k, wq, wk_ref[...].astype(bf16), dm)
    tokens = q_pack.shape[0]
    below = positions((tile, tile), 0) >= positions((tile, tile), 1)
    for i in range(tokens // tile):
        rows = slice(i * tile, (i + 1) * tile)
        numer = jnp.zeros((tile, v.shape[1]), f32)
        denom = jnp.zeros((tile, LANES), f32)
        for j in range(i + 1):
            cols = slice(j * tile, (j + 1) * tile)
            t = dot(q_pack[rows], k_pack[:, cols])
            weight = (0.5 * t) * t + 0.5
            if j == i:
                weight = jnp.where(below, weight, 0.0)
            for c in range(tile // LANES):
                denom = denom + weight[:, c * LANES : (c + 1) * LANES]
            numer = numer + dot(weight.astype(bf16), v[cols])
        numer_ref[h, rows, :] = numer
        denom_ref[h, rows, :] = denom


def gather_slots(me_ref, slots, scr):
    me = me_ref[0]
    size = slots[0].shape[0]
    for d, slot in enumerate(slots):
        scr[pl.ds(pl.multiple_of((me ^ d) * size, 8), size), :] = slot[...]


def scatter_slots(me_ref, slots, scr):
    size = slots[0].shape[0]
    for d, slot in enumerate(slots):
        slot[...] = scr[pl.ds(pl.multiple_of((me_ref[0] ^ d) * size, 8), size), :]


def join_kernel(n, backward, me_ref, *refs):
    far, got, outs = refs[: -2 * n], refs[-2 * n : -n], refs[-n:]

    def before(a, b):
        return a > b if backward else a < b

    me, mine = me_ref[0], me_ref[1]
    outer = jnp.zeros(outs[0].shape, f32)
    for d, piece in enumerate(far, 1):
        outer = outer + jnp.where(before(mine ^ d, mine), piece[...], 0.0)
    for d, out in enumerate(outs):
        total = outer
        for e, piece in enumerate(got):
            if e != d:
                total = total + jnp.where(before(me ^ e, me ^ d), piece[...], 0.0)
        out[...] = total


def head_rows(scr, dm, h):
    start = h * dm.rows
    return scr[pl.ds(start if isinstance(h, int) else pl.multiple_of(start, 8), dm.rows), :]


def forward_kernel(dm, scale, n, parts, me_ref, t_ref, *rest):
    intra, rest = rest[: 4 * len(parts)], rest[4 * len(parts) :]
    slots, (student_ref, g_ref, gd_ref), backs = rest[:n], rest[n : n + 3], rest[n + 3 : 2 * n + 3]
    scr, back_scr = rest[2 * n + 3 :]
    gather_slots(me_ref, slots, scr)
    for p, (h0, count) in enumerate(parts):
        for i in range(count):
            numer, denom, phi, phi_t = [ref[i] for ref in intra[4 * p : 4 * p + 4]]
            outs = forward_head(dm, scale, head_rows(scr, dm, h0 + i), t_ref[h0 + i], numer, denom, phi, phi_t)
            for ref, value in zip((student_ref, g_ref, gd_ref), outs):
                ref[h0 + i] = value
            back_scr[(h0 + i) * dm.rows : (h0 + i + 1) * dm.rows, :] = outs[3]
    scatter_slots(me_ref, backs, back_scr)


def forward_head(dm, scale, state, teacher, numer, part, phi, phi_t):
    hd = state.shape[1]
    s_pack = jnp.concatenate(split2(state), 1)
    s_pack = jnp.concatenate([s_pack, jnp.zeros((dm.lanes - dm.rows, 2 * hd), bf16)], 0)
    p1, p2 = split2(phi)
    prod = dot(p1, s_pack) + dot(p2, s_pack)
    numer = numer + (prod[:, :hd] + prod[:, hd:])
    weighted = phi * count_of(state, dm)
    for c in range(dm.lanes // LANES):
        part = part + weighted[:, c * LANES : (c + 1) * LANES]
    inv = 1.0 / jnp.sum(part, 1, keepdims=True)
    y = numer * inv
    g_out = scale * (y - teacher.astype(f32))
    g_numer = g_out * inv
    g_denom = -jnp.sum(g_out * y, 1, keepdims=True) * inv
    t1, t2 = split2(phi_t)
    g_pack = jnp.concatenate(split2(g_numer), 1)
    prod = dot(t1, g_pack) + dot(t2, g_pack)
    back = with_count(prod[:, :hd] + prod[:, hd:], jnp.sum(phi * g_denom, 0, keepdims=True), dm)
    return y.astype(bf16), g_numer, jnp.broadcast_to(g_denom, part.shape), back


def count_column(state, dm):
    row, lane = positions((dm.rows, dm.lanes), 0), positions((dm.rows, dm.lanes), 1)
    return jnp.sum(jnp.where(row == lane, count_of(state, dm), 0.0), 1, keepdims=True)


def backward_kernel(dm, tile, n, h0, me_ref, q_ref, k_ref, v_ref, wq_ref, wk_ref, g_ref, gd_ref, *rest):
    slots, (gk_ref, wgrad_ref, scr) = rest[:n], rest[n:]
    h = h0 + pl.program_id(0)
    q, k, v = q_ref[h], k_ref[h], v_ref.at[h]

    @pl.when(pl.program_id(0) == 0)
    def _():
        gather_slots(me_ref, slots, scr)
        wgrad_ref[...] = jnp.zeros_like(wgrad_ref)

    state = head_rows(scr, dm, h)
    wq = wq_ref[...].astype(bf16)
    q_pack, k_pack, k1, k2 = packs(q, k, wq, wk_ref[...].astype(bf16), dm)
    k_two = jnp.concatenate([k1, k2], 0)
    ext = dot(rolled(wq, dm), q, NT)
    w = dm.width
    q1, q2 = split2(ext[:w])
    q_two = jnp.concatenate([q1, q2], 0)
    g_numer = g_ref[h]
    g_hi = g_numer.astype(bf16)
    tokens = q.shape[0]
    below = positions((tile, tile), 0) >= positions((tile, tile), 1)
    count = tokens // tile
    g_k = [jnp.zeros((w, tile), f32) for _ in range(count)]
    g_q = []
    for i in range(count):
        rows = slice(i * tile, (i + 1) * tile)
        gd = gd_ref[h, rows, :]
        gd = jnp.concatenate([gd] * (tile // LANES), 1)
        total = jnp.zeros((w, tile), f32)
        for j in range(i + 1):
            cols = slice(j * tile, (j + 1) * tile)
            t = dot(q_pack[rows], k_pack[:, cols])
            score = (dot(g_hi[rows], v[cols], NT) + gd) * t
            if j == i:
                score = jnp.where(below, score, 0.0)
            hi, lo = split2(score)
            both = dot(k_two[:, cols], hi, NT)
            total = total + (both[:w] + both[w:]) + dot(k1[:, cols], lo, NT)
            both = dot(q_two[:, rows], hi)
            g_k[j] = g_k[j] + (both[:w] + both[w:]) + dot(q1[:, rows], lo)
        g_q.append(total)
    gk_ref[pl.program_id(0)] = jnp.concatenate(g_k, 1)
    first = positions((1, LANES), 1) == 0
    s_aug = jnp.concatenate([state, jnp.where(first, count_column(state, dm), 0.0)], 1)
    g_aug = jnp.concatenate([g_numer, jnp.where(first, gd_ref[h], 0.0)], 1)
    s1, s2 = split2(s_aug)
    a1, a2 = split2(g_aug)
    both = dot(jnp.concatenate([s1, s2], 0), a1, NT)
    g_phi = both[: dm.rows] + both[dm.rows :] + dot(s1, a2, NT)
    total = jnp.concatenate(g_q, 1) + feature_grad_t(ext, g_phi, dm)
    wgrad_ref[...] += dot(total.astype(bf16), q)


def key_kernel(dm, n, parts, me_ref, k_ref, v_ref, wk_ref, *rest):
    slots, backs, (out_ref, scr) = rest[:n], rest[n:-2], rest[-2:]
    gather_slots(me_ref, slots, scr)
    w = dm.width
    out_ref[:w] = functools.reduce(jnp.add, [g[...] for g in backs[1::2]])
    w_ext = rolled(wk_ref[...].astype(bf16), dm)
    grad = jnp.zeros((w, out_ref.shape[1]), f32)
    for (h0, count), gk_ref in zip(parts, backs[::2]):
        for i in range(count):
            k, v = k_ref[h0 + i], v_ref[h0 + i]
            state = head_rows(scr, dm, h0 + i)
            g_phi = dot(state.astype(bf16), v, NT) + count_column(state, dm)
            total = gk_ref[i] + feature_grad_t(dot(w_ext, k, NT), g_phi, dm)
            grad = grad + dot(total.astype(bf16), k)
    out_ref[w:] = grad


VMEM_LIMIT = 20 * 1024 * 1024
HBM = pl.BlockSpec(memory_space=pltpu.HBM)
VMEM = pl.BlockSpec(memory_space=pltpu.VMEM)
SMEM = pl.BlockSpec(memory_space=pltpu.SMEM)


def placed(args, specs):
    spaces = {id(HBM): pltpu.HBM, id(VMEM): pltpu.VMEM}
    return [
        pltpu.with_memory_space_constraint(a, spaces[id(s)]) if id(s) in spaces else a
        for a, s in zip(args, specs)
    ]


def call(body, grid, args, specs, outs, out_specs, scratch, flops):
    return pl.pallas_call(
        body,
        grid=grid,
        in_specs=specs,
        out_specs=out_specs,
        out_shape=outs,
        scratch_shapes=scratch,
        compiler_params=pltpu.CompilerParams(
            dimension_semantics=("arbitrary",) * len(grid), vmem_limit_bytes=VMEM_LIMIT
        ),
        cost_estimate=pl.CostEstimate(flops=flops, bytes_accessed=0, transcendentals=0),
    )(*placed(args, specs))


def shifted(array, axis, pairs):
    return lax.ppermute(array, axis, pairs)


def exchange(parts, axis):
    n = lax.axis_size(axis)
    got = []
    for d, part in enumerate(parts):
        got.append(part if d == 0 else shifted(part, axis, [(i, i ^ d) for i in range(n)]))
    return got


def carried(me, parts, backward):
    n, m = lax.axis_size("seq"), lax.axis_size("seg")
    got = exchange(parts, "seq")
    total = functools.reduce(jnp.add, got)
    far = exchange([total] * m, "seg")[1:]
    shape = pltpu.VMEM(parts[0].shape, f32)
    before = call(
        functools.partial(join_kernel, n, backward),
        (),
        (me, *far, *got),
        [SMEM] + [VMEM] * (n + m - 1),
        [shape] * n,
        [VMEM] * n,
        [],
        parts[0].size * n * n,
    )
    return exchange(before, "seq")


def summed(array):
    for axis in ("head", "seq", "seg"):
        n = lax.axis_size(axis)
        got = [shifted(array, axis, [(i, i ^ d) for i in range(n)]) for d in range(1, n)]
        array = functools.reduce(jnp.add, [array] + got)
    return array


INTRA_SPLIT = (2, 2)
BACK_SPLIT = (1, 2, 1)


def split_heads(heads, split):
    if heads % sum(split):
        return [(0, heads)]
    unit, at, out = heads // sum(split), 0, []
    for part in split:
        out.append((at, part * unit))
        at += part * unit
    return out


def shards(queries, keys, values, teacher, query_proj, key_proj):
    heads, tokens, hd = queries.shape
    dm = Dims(query_proj.shape[1])
    n = lax.axis_size("seq")
    heads_all = heads * lax.axis_size("head")
    tokens_all = tokens * n * lax.axis_size("seg")
    scale = 1.0 / math.sqrt(heads_all * tokens_all)
    tile = min(256, tokens)
    wq, wk = query_proj.T, key_proj.T
    me = jnp.stack([lax.axis_index("seq"), lax.axis_index("seg")]).astype(jnp.int32)
    slot_shape = pltpu.VMEM((heads * dm.rows // n, hd), f32)
    tok_shape = pltpu.VMEM((heads, tokens, hd), f32)
    lane_shape = pltpu.VMEM((heads, tokens, LANES), f32)
    grad_shape = pltpu.VMEM((dm.width, hd), f32)
    slots = [pltpu.VMEM((heads * dm.rows, hd), f32)]

    sources = (keys, values, queries, teacher, wk, wq)
    called = call(
        functools.partial(state_kernel, dm, n),
        (),
        (me, *sources),
        [SMEM] + [HBM] * len(sources),
        [slot_shape] * n + [pltpu.VMEM(a.shape, a.dtype) for a in sources],
        [VMEM] * (n + len(sources)),
        slots + [pltpu.SemaphoreType.DMA((2 * heads,)), pltpu.SemaphoreType.DMA((4,))],
        4 * heads * tokens * dm.rows * hd,
    )
    states, (keys, values, queries, teacher, wk, wq) = called[:n], called[n:]
    intra = []
    intra_parts = split_heads(heads, INTRA_SPLIT)
    for h0, count in intra_parts:
        shapes = [
            pltpu.VMEM((count, tokens, hd), f32),
            pltpu.VMEM((count, tokens, LANES), f32),
            pltpu.VMEM((count, tokens, dm.lanes), f32),
            pltpu.VMEM((count, dm.rows, tokens), f32),
        ]
        intra += call(
            functools.partial(intra_kernel, dm, tile, h0),
            (count,),
            (queries, keys, values, wq, wk),
            [VMEM] * 5,
            shapes,
            [VMEM] * len(shapes),
            [],
            4 * count * tokens * tokens * hd,
        )
    prev = carried(me, states, False)
    student, g_numer, g_denom, *back = call(
        functools.partial(forward_kernel, dm, scale, n, intra_parts),
        (),
        (me, teacher, *intra, *prev),
        [SMEM] + [VMEM] * (1 + len(intra) + n),
        [pltpu.VMEM((heads, tokens, hd), bf16), tok_shape, lane_shape] + [slot_shape] * n,
        [VMEM] * (3 + n),
        2 * slots,
        8 * heads * tokens * dm.lanes * hd,
    )
    backs = []
    back_parts = split_heads(heads, BACK_SPLIT)
    for h0, count in back_parts:
        backs += call(
            functools.partial(backward_kernel, dm, tile, n, h0),
            (count,),
            (me, queries, keys, values, wq, wk, g_numer, g_denom, *prev),
            [SMEM] + [VMEM] * (7 + n),
            [pltpu.VMEM((count, dm.width, tokens), f32), grad_shape],
            [VMEM, VMEM],
            slots,
            8 * count * tokens * tokens * hd,
        )
    later = carried(me, back, True)
    grads = call(
        functools.partial(key_kernel, dm, n, back_parts),
        (),
        (me, keys, values, wk, *later, *backs),
        [SMEM] + [VMEM] * (3 + n + len(backs)),
        [pltpu.VMEM((2 * dm.width, hd), f32)],
        [VMEM],
        slots,
        4 * heads * tokens * dm.rows * hd,
    )[0]
    grads = summed(grads)
    return student, grads[: dm.width].T, grads[dm.width :].T


def solution(mesh):
    in_specs = (
        P("head", ("seg", "seq"), None),
        P("head", ("seg", "seq"), None),
        P("head", ("seg", "seq"), None),
        P("head", ("seg", "seq"), None),
        P(),
        P(),
    )
    out_specs = (P("head", ("seg", "seq"), None), P(), P())
    return jax.shard_map(shards, mesh=mesh, in_specs=in_specs, out_specs=out_specs, check_vma=False)
```

```python
import functools
import math

import jax
import jax.numpy as jnp
from jax import lax
from jax.experimental import pallas as pl
from jax.experimental.pallas import tpu as pltpu
from jax.sharding import PartitionSpec as P

f32 = jnp.float32
bf16 = jnp.bfloat16
HALF = 0.5**0.5
LANES = 128
NT = (((1,), (1,)), ((), ()))


class Dims:
    def __init__(self, width):
        self.width = width
        self.half = width // 2
        self.shift = width.bit_length() - 1
        assert width == 1 << self.shift
        self.quad = width * (width + 1) // 2
        self.lin = self.quad
        self.const = self.quad + width
        self.feats = self.const + 1
        self.lanes = -(-self.feats // LANES) * LANES
        self.count_rows = self.lanes // LANES
        self.rows = -(-(self.feats + self.count_rows) // 8) * 8


def positions(shape, dim):
    return lax.broadcasted_iota(jnp.int32, shape, dim)


def one_hot(hit):
    return jnp.where(hit, 1.0, 0.0).astype(bf16)


def first_of(dm, f):
    return jnp.where(f < dm.quad, f & (dm.width - 1), f - dm.lin)


def second_of(dm, f):
    return (f + (f >> dm.shift)) & (dm.width - 1)


def tiles(tokens, size=256):
    size = min(size, tokens)
    return [slice(i, i + size) for i in range(0, tokens, size)]


def dot(a, b, dims=(((1,), (0,)), ((), ()))):
    return lax.dot_general(a, b, dims, preferred_element_type=f32)


def split2(x):
    hi = x.astype(bf16)
    return hi, (x - hi.astype(f32)).astype(bf16)


def split3(x):
    hi = x.astype(bf16)
    rest = x - hi.astype(f32)
    mid = rest.astype(bf16)
    return hi, mid, (rest - mid.astype(f32)).astype(bf16)


def rolled(w_t, dm):
    shape = (dm.quad, dm.width)
    return dot(one_hot(second_of(dm, positions(shape, 0)) == positions(shape, 1)), w_t).astype(bf16)


def repeated(w_t, dm):
    shape = (LANES, dm.width)
    return dot(one_hot((positions(shape, 0) & (dm.width - 1)) == positions(shape, 1)), w_t).astype(bf16)


def sides(w_t, dm):
    shape = (dm.lanes, dm.width)
    f, j = positions(shape, 0), positions(shape, 1)
    left = dot(one_hot(first_of(dm, f) == j), w_t).astype(bf16)
    right = dot(one_hot((f < dm.quad) & (second_of(dm, f) == j)), w_t).astype(bf16)
    return left, right


def features_t(ext, dm):
    w = dm.width
    base = ext[:w]
    parts = [HALF * base * base]
    for d in range(1, dm.half):
        parts.append(ext[d * w : (d + 1) * w] * base)
    parts.append(ext[dm.half * w : dm.quad] * base[: dm.half])
    parts.append(base)
    tail = dm.rows - dm.const
    rows = lax.broadcasted_iota(jnp.int32, (tail, ext.shape[1]), 0)
    parts.append(jnp.where(rows == 0, 1.0, 0.0).astype(f32))
    return jnp.concatenate(parts, 0)


def features_rows(rows, side, dm):
    left, right = side
    f = positions((1, dm.lanes), 1)
    left = dot(rows, left, NT) + jnp.where(f == dm.const, 1.0, 0.0)
    right = dot(rows, right, NT) + jnp.where((f >= dm.lin) & (f < dm.feats), 1.0, 0.0)
    return jnp.where(f < dm.width, HALF, 1.0) * left * right


def feature_grad_t(ext, g, dm):
    w, half = dm.width, dm.half
    base = ext[:w]
    total = g[dm.lin : dm.lin + w] + (2.0 * HALF) * g[:w] * base
    for d in range(1, half):
        quad = g[d * w : (d + 1) * w]
        total = total + quad * ext[d * w : (d + 1) * w]
        back = quad * base
        total = total + jnp.concatenate([back[w - d :], back[: w - d]], 0)
    quad = g[half * w : dm.quad]
    return total + jnp.concatenate([quad * base[half:], quad * base[:half]], 0)


def with_count(state, count, dm):
    rows = lax.broadcasted_iota(jnp.int32, state.shape, 0)
    for c in range(dm.count_rows):
        state = jnp.where(rows == dm.feats + c, count[:, c * LANES : (c + 1) * LANES], state)
    return state


def count_of(state, dm):
    return jnp.concatenate([state[dm.feats + c : dm.feats + c + 1] for c in range(dm.count_rows)], 1)


def column_row(part, dm):
    column = jnp.sum(part, 1, keepdims=True)
    row, lane = positions((dm.rows, dm.lanes), 0), positions((dm.rows, dm.lanes), 1)
    return jnp.sum(jnp.where(row == lane, column, 0.0), 0, keepdims=True)


def state_kernel(dm, n, me_ref, *rest):
    sources, slots, kept, at_ref, scr, sems = rest[:4], rest[4 : 4 + n], rest[4 + n : 8 + n], *rest[8 + n :]
    at_ref[0] = me_ref[0]
    at_ref[1] = me_ref[1]
    wk_ref, k_ref, v_ref = kept[:3]
    heads = k_ref.shape[0]
    copies = [pltpu.make_async_copy(a, b, sems.at[i]) for i, (a, b) in enumerate(zip(sources, kept))]
    for copy in copies:
        copy.start()
    copies[0].wait()
    w_ext = rolled(wk_ref[...].astype(bf16), dm)
    for copy in copies[1:]:
        copy.wait()
    for h in range(heads):
        phi = features_t(dot(w_ext, k_ref[h], NT), dm)
        part = phi[:, :LANES]
        for c in range(LANES, phi.shape[1], LANES):
            part = part + phi[:, c : c + LANES]
        state = dot(phi.astype(bf16), v_ref[h])
        scr[h * dm.rows : (h + 1) * dm.rows, :] = with_count(state, column_row(part, dm), dm)
    scatter_slots(me_ref, slots, scr)


def turn_kernel(v_ref, q_hbm, t_hbm, vt_ref, q_ref, t_ref, sems):
    copies = [pltpu.make_async_copy(a, b, sems.at[i]) for i, (a, b) in enumerate(((q_hbm, q_ref), (t_hbm, t_ref)))]
    for copy in copies:
        copy.start()
    for h in range(v_ref.shape[0]):
        vt_ref[h] = v_ref[h].T
    for copy in copies:
        copy.wait()


def packs(q, k, wq, wk, dm):
    w = dm.width
    q1, q2, q3 = split3(dot(q, repeated(wq, dm), NT))
    group = positions((1, LANES), 1)
    zero = jnp.zeros((), bf16)

    def at(lo, hi):
        return (group >= lo * w) & (group < hi * w)

    q_pack = jnp.where(at(0, 3), q1, jnp.where(at(3, 5), q2, jnp.where(at(5, 6), q3, zero)))
    q_pack = jnp.where(group == 6 * w, jnp.ones((), bf16), q_pack)
    k_t = dot(wk, k, NT)
    k1, k2, k3 = split3(k_t)
    last = one_hot(positions((LANES - 6 * w, k_t.shape[1]), 0) == 0)
    return q_pack, jnp.concatenate([k1, k2, k3, k1, k2, k1, last], 0)


def intra_kernel(dm, tile, h0, q_ref, k_ref, v_ref, wq_ref, wk_ref, *outs):
    numer_ref, denom_ref, q_pack_ref, k_pack_ref, q_two_ref, ext_ref = outs
    h = pl.program_id(0)
    q, k, v = q_ref[h0 + h], k_ref[h0 + h], v_ref.at[h0 + h]
    wq = wq_ref[...].astype(bf16)
    ext = dot(rolled(wq, dm), q, NT)
    ext_ref[h] = ext
    q_two_ref[h] = jnp.concatenate(split2(ext[: dm.width]), 0)
    q_pack, k_pack = packs(q, k, wq, wk_ref[...].astype(bf16), dm)
    q_pack_ref[h] = q_pack
    k_pack_ref[h] = k_pack
    tokens = q_pack.shape[0]
    below = positions((tile, tile), 0) >= positions((tile, tile), 1)
    for i in range(tokens // tile):
        rows = slice(i * tile, (i + 1) * tile)
        numer = jnp.zeros((tile, v.shape[1]), f32)
        denom = jnp.zeros((tile, LANES), f32)
        for j in range(i + 1):
            cols = slice(j * tile, (j + 1) * tile)
            t = dot(q_pack[rows], k_pack[:, cols])
            weight = (0.5 * t) * t + 0.5
            if j == i:
                weight = jnp.where(below, weight, 0.0)
            for c in range(tile // LANES):
                denom = denom + weight[:, c * LANES : (c + 1) * LANES]
            numer = numer + dot(weight.astype(bf16), v[cols])
        numer_ref[h, rows, :] = numer
        denom_ref[h, rows, :] = denom


def feature_kernel(dm, h0, q_ref, wq_ref, ext_ref, phi_ref, p1_ref, p2_ref, t_ref):
    h = pl.program_id(0)
    wq = wq_ref[...].astype(bf16)
    side = sides(wq, dm)
    for cols in tiles(q_ref.shape[1]):
        phi = features_rows(q_ref[h0 + h, cols, :], side, dm)
        phi_ref[h, cols, :] = phi
        p1_ref[h, cols, :], p2_ref[h, cols, :] = split2(phi)
        t_ref[h, :, cols] = jnp.concatenate(split2(features_t(ext_ref[h, :, cols], dm)), 0)


def gather_slots(me_ref, slots, scr):
    me = me_ref[0]
    size = slots[0].shape[0]
    for d, slot in enumerate(slots):
        scr[pl.ds(pl.multiple_of((me ^ d) * size, 8), size), :] = slot[...]


def scatter_slots(me_ref, slots, scr):
    size = slots[0].shape[0]
    for d, slot in enumerate(slots):
        slot[...] = scr[pl.ds(pl.multiple_of((me_ref[0] ^ d) * size, 8), size), :]


def join_kernel(n, backward, me_ref, *refs):
    far, got, outs = refs[: -2 * n], refs[-2 * n : -n], refs[-n:]

    def before(a, b):
        return a > b if backward else a < b

    me, mine = me_ref[0], me_ref[1]
    outer = jnp.zeros(outs[0].shape, f32)
    for d, piece in enumerate(far, 1):
        outer = outer + jnp.where(before(mine ^ d, mine), piece[...], 0.0)
    for d, out in enumerate(outs):
        total = outer
        for e, piece in enumerate(got):
            if e != d:
                total = total + jnp.where(before(me ^ e, me ^ d), piece[...], 0.0)
        out[...] = total


def head_rows(scr, dm, h):
    start = h * dm.rows
    return scr[pl.ds(start if isinstance(h, int) else pl.multiple_of(start, 8), dm.rows), :]


def forward_kernel(dm, scale, n, parts, me_ref, t_ref, *rest):
    used, rest = rest[: 6 * len(parts)], rest[6 * len(parts) :]
    slots, outs, backs = rest[:n], rest[n : n + 3], rest[n + 3 : 2 * n + 3]
    scr, back_scr = rest[2 * n + 3 :]
    gather_slots(me_ref, slots, scr)
    for p, (h0, count) in enumerate(parts):
        for i in range(count):
            h = h0 + i
            refs = [ref.at[i] for ref in used[6 * p : 6 * p + 6]]
            back = forward_head(dm, scale, head_rows(scr, dm, h), t_ref.at[h], *refs, *[ref.at[h] for ref in outs])
            back_scr[h * dm.rows : (h + 1) * dm.rows, :] = back
    scatter_slots(me_ref, backs, back_scr)


def forward_head(
    dm, scale, state, teacher, numer_ref, denom_ref, phi_ref, p1_ref, p2_ref, phi_t_ref, student_ref, g_ref, gd_ref
):
    hd = state.shape[1]
    s_pack = jnp.concatenate(split2(state), 1)
    s_pack = jnp.concatenate([s_pack, jnp.zeros((dm.lanes - dm.rows, 2 * hd), bf16)], 0)
    before = count_of(state, dm)
    back, count = 0.0, 0.0
    for rows in tiles(teacher.shape[0]):
        phi = phi_ref[rows]
        prod = dot(p1_ref[rows], s_pack) + dot(p2_ref[rows], s_pack)
        numer = numer_ref[rows] + (prod[:, :hd] + prod[:, hd:])
        weighted = phi * before
        part = denom_ref[rows]
        for c in range(0, dm.lanes, LANES):
            part = part + weighted[:, c : c + LANES]
        inv = 1.0 / jnp.sum(part, 1, keepdims=True)
        y = numer * inv
        student_ref[rows] = y.astype(bf16)
        g_out = scale * (y - teacher[rows].astype(f32))
        g_numer = g_out * inv
        g_denom = -jnp.sum(g_out * y, 1, keepdims=True) * inv
        g_ref[rows] = g_numer
        gd_ref[rows] = jnp.broadcast_to(g_denom, part.shape)
        count = count + jnp.sum(phi * g_denom, 0, keepdims=True)
        back = back + dot(phi_t_ref[:, rows], jnp.concatenate(split2(g_numer), 1))
    back = back[: dm.rows] + back[dm.rows :]
    return with_count(back[:, :hd] + back[:, hd:], count, dm)


def count_column(state, dm):
    row, lane = positions((dm.rows, dm.lanes), 0), positions((dm.rows, dm.lanes), 1)
    return jnp.sum(jnp.where(row == lane, count_of(state, dm), 0.0), 1, keepdims=True)


def backward_kernel(dm, tile, n, h0, me_ref, q_ref, vt_ref, g_ref, gd_ref, q_pack_ref, k_pack_ref, q_two_ref, ext_ref, *rest):
    slots, (gk_ref, wgrad_ref, scr) = rest[:n], rest[n : n + 3]
    i0 = pl.program_id(0)
    h = h0 + i0

    @pl.when(i0 == 0)
    def _():
        gather_slots(me_ref, slots, scr)
        wgrad_ref[...] = jnp.zeros_like(wgrad_ref)

    state = head_rows(scr, dm, h)
    w = dm.width
    q_pack, k_pack, q_two, vt = q_pack_ref.at[i0], k_pack_ref.at[i0], q_two_ref.at[i0], vt_ref.at[h]
    g_numer, g_denom, ext = g_ref.at[h], gd_ref.at[h], ext_ref.at[i0]
    s_aug = jnp.concatenate(
        [state, jnp.where(positions((1, LANES), 1) == 0, count_column(state, dm), 0.0)], 1
    )
    s1, s2 = split2(s_aug)
    s_two = jnp.concatenate([s1, s2], 0)
    count = q_pack.shape[0] // tile
    below = positions((tile, tile), 0) >= positions((tile, tile), 1)
    g_q, g_k = [], 0.0
    for i in range(count):
        rows = slice(i * tile, (i + 1) * tile)
        width = (i + 1) * tile
        t = dot(q_pack[rows], k_pack[:, :width])
        g_weight = dot(g_numer[rows].astype(bf16), vt[:, :width]) + jnp.concatenate([g_denom[rows]] * (width // LANES), 1)
        score = g_weight * t
        last = jnp.where(below, score[:, width - tile :], 0.0)
        hi, lo = split2(jnp.concatenate([score[:, : width - tile], last], 1) if i else last)
        both = dot(k_pack[: 2 * w, :width], hi, NT)
        g_q.append(both[:w] + both[w:] + dot(k_pack[:w, :width], lo, NT))
        both = dot(q_two[:, rows], hi)
        part = both[:w] + both[w:] + dot(q_two[:w, rows], lo)
        rest = count * tile - width
        g_k = g_k + (jnp.concatenate([part, jnp.zeros((w, rest), f32)], 1) if rest else part)
    gk_ref[i0] = g_k
    first = positions((1, LANES), 1) == 0
    a1, a2 = split2(jnp.concatenate([g_numer[...], jnp.where(first, g_denom[...], 0.0)], 1))
    both = dot(s_two, a1, NT)
    g_phi = both[: dm.rows] + both[dm.rows :] + dot(s1, a2, NT)
    total = jnp.concatenate(g_q, 1) + feature_grad_t(ext[...], g_phi, dm)
    wgrad_ref[...] += dot(total.astype(bf16), q_ref[h])


def saving_kernel(body, n_in, *refs):
    src, dst, sem = refs[n_in - 1], refs[-3], refs[-1]
    copy = pltpu.make_async_copy(src, dst, sem.at[0])
    pl.when(pl.program_id(0) == 0)(copy.start)
    body(*refs[: n_in - 1], *refs[n_in:-3], refs[-2])
    pl.when(pl.program_id(0) == pl.num_programs(0) - 1)(copy.wait)


def key_kernel(dm, n, parts, me_ref, k_ref, vt_ref, wk_ref, *rest):
    slots, backs, (out_ref, scr) = rest[:n], rest[n:-2], rest[-2:]
    gather_slots(me_ref, slots, scr)
    w = dm.width
    out_ref[:w] = functools.reduce(jnp.add, [g[...] for g in backs[1::2]])
    w_ext = rolled(wk_ref[...].astype(bf16), dm)
    grad = jnp.zeros((w, out_ref.shape[1]), f32)
    for (h0, count), gk_ref in zip(parts, backs[::2]):
        for i in range(count):
            state = head_rows(scr, dm, h0 + i)
            column, state = count_column(state, dm), state.astype(bf16)
            k = k_ref[h0 + i]
            g_phi = dot(state, vt_ref[h0 + i]) + column
            total = gk_ref[i] + feature_grad_t(dot(w_ext, k, NT), g_phi, dm)
            grad = grad + dot(total.astype(bf16), k)
    out_ref[w:] = grad


VMEM_LIMIT = 20 * 1024 * 1024
HBM = pl.BlockSpec(memory_space=pltpu.HBM)
VMEM = pl.BlockSpec(memory_space=pltpu.VMEM)
SMEM = pl.BlockSpec(memory_space=pltpu.SMEM)


def placed(args, specs):
    spaces = {id(HBM): pltpu.HBM, id(VMEM): pltpu.VMEM, id(SMEM): pltpu.SMEM}
    return [
        pltpu.with_memory_space_constraint(a, spaces[id(s)]) if id(s) in spaces else a
        for a, s in zip(args, specs)
    ]


def call(body, grid, args, specs, outs, out_specs, scratch, flops):
    return pl.pallas_call(
        body,
        grid=grid,
        in_specs=specs,
        out_specs=out_specs,
        out_shape=outs,
        scratch_shapes=scratch,
        compiler_params=pltpu.CompilerParams(
            dimension_semantics=("arbitrary",) * len(grid), vmem_limit_bytes=VMEM_LIMIT
        ),
        cost_estimate=pl.CostEstimate(flops=flops, bytes_accessed=0, transcendentals=0),
    )(*placed(args, specs))


def shifted(array, axis, pairs):
    return lax.ppermute(array, axis, pairs)


def exchange(parts, axis):
    n = lax.axis_size(axis)
    got = []
    for d, part in enumerate(parts):
        got.append(part if d == 0 else shifted(part, axis, [(i, i ^ d) for i in range(n)]))
    return got


def carried(me, parts, backward):
    n, m = lax.axis_size("seq"), lax.axis_size("seg")
    got = exchange(parts, "seq")
    total = functools.reduce(jnp.add, got)
    far = exchange([total] * m, "seg")[1:]
    shape = pltpu.VMEM(parts[0].shape, f32)
    before = call(
        functools.partial(join_kernel, n, backward),
        (),
        (me, *far, *got),
        [SMEM] + [VMEM] * (n + m - 1),
        [shape] * n,
        [VMEM] * n,
        [],
        parts[0].size * n * n,
    )
    return exchange(before, "seq")


def summed(array):
    for axis in ("head", "seq", "seg"):
        array = functools.reduce(jnp.add, exchange([array] * lax.axis_size(axis), axis))
    return array


SPLIT = (1, 2, 1)


def split_heads(heads, split):
    if heads % sum(split):
        return [(0, heads)]
    unit, at, out = heads // sum(split), 0, []
    for part in split:
        out.append((at, part * unit))
        at += part * unit
    return out


def shards(queries, keys, values, teacher, query_proj, key_proj):
    heads, tokens, hd = queries.shape
    dm = Dims(query_proj.shape[1])
    n = lax.axis_size("seq")
    heads_all = heads * lax.axis_size("head")
    tokens_all = tokens * n * lax.axis_size("seg")
    scale = 1.0 / math.sqrt(heads_all * tokens_all)
    tile = min(256, tokens)
    wq, wk = query_proj.T, key_proj.T
    me = jnp.stack([lax.axis_index("seq"), lax.axis_index("seg")]).astype(jnp.int32)
    slot_shape = pltpu.VMEM((heads * dm.rows // n, hd), f32)
    tok_shape = pltpu.VMEM((heads, tokens, hd), f32)
    lane_shape = pltpu.VMEM((heads, tokens, LANES), f32)
    grad_shape = pltpu.VMEM((dm.width, hd), f32)
    slots = [pltpu.VMEM((heads * dm.rows, hd), f32)]

    sources = (wk, keys, values, wq)
    called = call(
        functools.partial(state_kernel, dm, n),
        (),
        (me, *sources),
        [SMEM] + [HBM] * len(sources),
        [slot_shape] * n + [pltpu.VMEM(a.shape, a.dtype) for a in sources] + [pltpu.SMEM((2,), jnp.int32)],
        [VMEM] * (n + len(sources)) + [SMEM],
        slots + [pltpu.SemaphoreType.DMA((len(sources),))],
        4 * heads * tokens * dm.rows * hd,
    )
    states, (wk, keys, values, wq, me) = called[:n], called[n:]
    vt, queries, teacher = call(
        turn_kernel,
        (),
        (values, queries, teacher),
        [VMEM, HBM, HBM],
        [pltpu.VMEM((heads, hd, tokens), bf16)] + [pltpu.VMEM(a.shape, bf16) for a in (queries, teacher)],
        [VMEM] * 3,
        [pltpu.SemaphoreType.DMA((2,))],
        heads * tokens * hd * hd,
    )
    intra, packed, intra_parts = [], [], split_heads(heads, SPLIT)
    for h0, count in intra_parts:
        outs = call(
            functools.partial(intra_kernel, dm, tile, h0),
            (count,),
            (queries, keys, values, wq, wk),
            [VMEM] * 5,
            [
                pltpu.VMEM((count, tokens, hd), f32),
                pltpu.VMEM((count, tokens, LANES), f32),
                pltpu.VMEM((count, tokens, LANES), bf16),
                pltpu.VMEM((count, LANES, tokens), bf16),
                pltpu.VMEM((count, 2 * dm.width, tokens), bf16),
                pltpu.VMEM((count, dm.quad, tokens), f32),
            ],
            [VMEM] * 6,
            [],
            4 * count * tokens * tokens * hd,
        )
        outs += call(
            functools.partial(feature_kernel, dm, h0),
            (count,),
            (queries, wq, outs[5]),
            [VMEM] * 3,
            [
                pltpu.VMEM((count, tokens, dm.lanes), f32),
                pltpu.VMEM((count, tokens, dm.lanes), bf16),
                pltpu.VMEM((count, tokens, dm.lanes), bf16),
                pltpu.VMEM((count, 2 * dm.rows, tokens), bf16),
            ],
            [VMEM] * 4,
            [],
            4 * count * tokens * dm.lanes * hd,
        )
        intra += outs[:2] + outs[6:]
        packed.append(outs[2:6])
    prev = carried(me, states, False)
    student, g_numer, g_denom, *back = call(
        functools.partial(forward_kernel, dm, scale, n, intra_parts),
        (),
        (me, teacher, *intra, *prev),
        [SMEM] + [VMEM] * (1 + len(intra) + n),
        [pltpu.VMEM((heads, tokens, hd), bf16), tok_shape, lane_shape] + [slot_shape] * n,
        [VMEM] * (3 + n),
        2 * slots,
        8 * heads * tokens * dm.lanes * hd,
    )
    backs = []
    for part, (h0, count) in enumerate(intra_parts):
        body = functools.partial(backward_kernel, dm, tile, n, h0)
        args = (me, queries, vt, g_numer, g_denom, *packed[part], *prev)
        outs = [pltpu.VMEM((count, dm.width, tokens), f32), grad_shape]
        specs, scratch = [VMEM] * len(outs), slots
        if part == 0:
            args += (student,)
            body = functools.partial(saving_kernel, body, len(args))
            outs, specs = outs + [pltpu.HBM(student.shape, bf16)], specs + [HBM]
            scratch = slots + [pltpu.SemaphoreType.DMA((1,))]
        outs = call(
            body,
            (count,),
            args,
            [SMEM] + [VMEM] * (len(args) - 1),
            outs,
            specs,
            scratch,
            8 * count * tokens * tokens * hd,
        )
        if part == 0:
            student = outs[2]
        backs += outs[:2]
    later = carried(me, back, True)
    grads = call(
        functools.partial(key_kernel, dm, n, intra_parts),
        (),
        (me, keys, vt, wk, *later, *backs),
        [SMEM] + [VMEM] * (3 + n + len(backs)),
        [pltpu.VMEM((2 * dm.width, hd), f32)],
        [VMEM],
        slots,
        4 * heads * tokens * dm.rows * hd,
    )[0]
    grads = summed(grads)
    return student, grads[: dm.width].T, grads[dm.width :].T


def solution(mesh):
    in_specs = (
        P("head", ("seg", "seq"), None),
        P("head", ("seg", "seq"), None),
        P("head", ("seg", "seq"), None),
        P("head", ("seg", "seq"), None),
        P(),
        P(),
    )
    out_specs = (P("head", ("seg", "seq"), None), P(), P())
    return jax.shard_map(shards, mesh=mesh, in_specs=in_specs, out_specs=out_specs, check_vma=False)
```

```python
import functools
import math

import jax
import jax.numpy as jnp
from jax import lax
from jax.experimental import pallas as pl
from jax.experimental.pallas import tpu as pltpu
from jax.sharding import PartitionSpec as P


f32 = jnp.float32
bf16 = jnp.bfloat16
HALF = 0.5**0.5
LANES = 128
NT = (((1,), (1,)), ((), ()))


class Dims:
    def __init__(self, width):
        self.width = width
        self.half = width // 2
        self.shift = width.bit_length() - 1
        assert width == 1 << self.shift
        self.quad = width * (width + 1) // 2
        self.lin = self.quad
        self.const = self.quad + width
        self.feats = self.const + 1
        self.lanes = -(-self.feats // LANES) * LANES
        self.count_rows = self.lanes // LANES
        self.rows = -(-(self.feats + self.count_rows) // 8) * 8


def positions(shape, dim):
    return lax.broadcasted_iota(jnp.int32, shape, dim)


def one_hot(hit):
    return jnp.where(hit, 1.0, 0.0).astype(bf16)


def first_of(dm, f):
    return jnp.where(f < dm.quad, f & (dm.width - 1), f - dm.lin)


def second_of(dm, f):
    return (f + (f >> dm.shift)) & (dm.width - 1)


def tiles(tokens, size=256):
    size = min(size, tokens)
    return [slice(i, i + size) for i in range(0, tokens, size)]


def dot(a, b, dims=(((1,), (0,)), ((), ()))):
    return lax.dot_general(a, b, dims, preferred_element_type=f32)


def split2(x):
    hi = x.astype(bf16)
    return hi, (x - hi.astype(f32)).astype(bf16)


def split3(x):
    hi = x.astype(bf16)
    rest = x - hi.astype(f32)
    mid = rest.astype(bf16)
    return hi, mid, (rest - mid.astype(f32)).astype(bf16)


def rolled(w_t, dm):
    shape = (dm.quad, dm.width)
    return dot(one_hot(second_of(dm, positions(shape, 0)) == positions(shape, 1)), w_t).astype(bf16)


def repeated(w_t, dm):
    shape = (LANES, dm.width)
    return dot(one_hot((positions(shape, 0) & (dm.width - 1)) == positions(shape, 1)), w_t).astype(bf16)


def sides(w_t, dm):
    shape = (dm.lanes, dm.width)
    f, j = positions(shape, 0), positions(shape, 1)
    left = dot(one_hot(first_of(dm, f) == j), w_t).astype(bf16)
    right = dot(one_hot((f < dm.quad) & (second_of(dm, f) == j)), w_t).astype(bf16)
    return left, right


def features_t(ext, dm):
    w = dm.width
    base = ext[:w]
    parts = [HALF * base * base]
    for d in range(1, dm.half):
        parts.append(ext[d * w : (d + 1) * w] * base)
    parts.append(ext[dm.half * w : dm.quad] * base[: dm.half])
    parts.append(base)
    tail = dm.rows - dm.const
    rows = lax.broadcasted_iota(jnp.int32, (tail, ext.shape[1]), 0)
    parts.append(jnp.where(rows == 0, 1.0, 0.0).astype(f32))
    return jnp.concatenate(parts, 0)


def features_rows(rows, side, dm):
    left, right = side
    f = positions((1, dm.lanes), 1)
    left = dot(rows, left, NT) + jnp.where(f == dm.const, 1.0, 0.0)
    right = dot(rows, right, NT) + jnp.where((f >= dm.lin) & (f < dm.feats), 1.0, 0.0)
    return jnp.where(f < dm.width, HALF, 1.0) * left * right


def feature_grad_t(ext, g, dm):
    w, half = dm.width, dm.half
    base = ext[:w]
    total = g[dm.lin : dm.lin + w] + (2.0 * HALF) * g[:w] * base
    for d in range(1, half):
        quad = g[d * w : (d + 1) * w]
        total = total + quad * ext[d * w : (d + 1) * w]
        back = quad * base
        total = total + jnp.concatenate([back[w - d :], back[: w - d]], 0)
    quad = g[half * w : dm.quad]
    return total + jnp.concatenate([quad * base[half:], quad * base[:half]], 0)


def with_count(state, count, dm):
    rows = lax.broadcasted_iota(jnp.int32, state.shape, 0)
    for c in range(dm.count_rows):
        state = jnp.where(rows == dm.feats + c, count[:, c * LANES : (c + 1) * LANES], state)
    return state


def count_of(state, dm):
    return jnp.concatenate([state[dm.feats + c : dm.feats + c + 1] for c in range(dm.count_rows)], 1)


def column_row(part, dm):
    column = jnp.sum(part, 1, keepdims=True)
    row, lane = positions((dm.rows, dm.lanes), 0), positions((dm.rows, dm.lanes), 1)
    return jnp.sum(jnp.where(row == lane, column, 0.0), 0, keepdims=True)


def head_at(me_ref, per, p):
    return (me_ref[0] >> (per.bit_length() - 1)) ^ p


def put_slots(me_ref, slots, scr, value):
    if len(slots) == 1:
        slots[0][...] = value
        return
    scr[...] = value
    size = slots[0].shape[0]
    for c, slot in enumerate(slots):
        slot[...] = scr[pl.ds(pl.multiple_of(((me_ref[0] & (len(slots) - 1)) ^ c) * size, 8), size), :]


def get_slots(me_ref, slots, scr):
    if len(slots) == 1:
        return slots[0][...]
    size = slots[0].shape[0]
    for c, slot in enumerate(slots):
        scr[pl.ds(pl.multiple_of(((me_ref[0] & (len(slots) - 1)) ^ c) * size, 8), size), :] = slot[...]
    return scr[...]


def state_kernel(dm, n, me_ref, *rest):
    sources, slots, kept, at_ref, scr, sems = rest[:4], rest[4 : 4 + n], rest[4 + n : 8 + n], *rest[8 + n :]
    at_ref[0] = me_ref[0]
    at_ref[1] = me_ref[1]
    wk_ref, k_ref, v_ref = kept[:3]
    heads = k_ref.shape[0]
    per = n // heads
    copies = [pltpu.make_async_copy(a, b, sems.at[i]) for i, (a, b) in enumerate(zip(sources, kept))]
    for copy in copies:
        copy.start()
    copies[0].wait()
    w_ext = rolled(wk_ref[...].astype(bf16), dm)
    copies[1].wait()
    phis, parts = [], []
    for p in range(heads):
        phi = features_t(dot(w_ext, k_ref[head_at(me_ref, per, p)], NT), dm)
        part = phi[:, :LANES]
        for c in range(LANES, phi.shape[1], LANES):
            part = part + phi[:, c : c + LANES]
        phis.append(phi.astype(bf16))
        parts.append(part)
    for copy in copies[2:]:
        copy.wait()
    for p in range(heads):
        state = with_count(dot(phis[p], v_ref[head_at(me_ref, per, p)]), column_row(parts[p], dm), dm)
        put_slots(me_ref, slots[p * per : (p + 1) * per], scr, state)


def turn_kernel(v_ref, q_hbm, t_hbm, vt_ref, q_ref, t_ref, sems):
    copies = [pltpu.make_async_copy(a, b, sems.at[i]) for i, (a, b) in enumerate(((q_hbm, q_ref), (t_hbm, t_ref)))]
    for copy in copies:
        copy.start()
    for h in range(v_ref.shape[0]):
        vt_ref[h] = v_ref[h].T
    for copy in copies:
        copy.wait()


def packs(q, k, wq, wk, dm):
    w = dm.width
    q1, q2, q3 = split3(dot(q, repeated(wq, dm), NT))
    group = positions((1, LANES), 1)
    zero = jnp.zeros((), bf16)

    def at(lo, hi):
        return (group >= lo * w) & (group < hi * w)

    q_pack = jnp.where(at(0, 3), q1, jnp.where(at(3, 5), q2, jnp.where(at(5, 6), q3, zero)))
    q_pack = jnp.where(group == 6 * w, jnp.ones((), bf16), q_pack)
    k_t = dot(wk, k, NT)
    k1, k2, k3 = split3(k_t)
    last = one_hot(positions((LANES - 6 * w, k_t.shape[1]), 0) == 0)
    return q_pack, jnp.concatenate([k1, k2, k3, k1, k2, k1, last], 0)


def intra_kernel(dm, tile, per, p0, me_ref, q_ref, k_ref, v_ref, wq_ref, wk_ref, *outs):
    numer_ref, denom_ref, q_pack_ref, k_pack_ref, q_two_ref, ext_ref = outs
    h = pl.program_id(0)
    at = head_at(me_ref, per, p0 + h)
    q, k, v = q_ref[at], k_ref[at], v_ref.at[at]
    wq = wq_ref[...].astype(bf16)
    ext = dot(rolled(wq, dm), q, NT)
    ext_ref[h] = ext
    q_two_ref[h] = jnp.concatenate(split2(ext[: dm.width]), 0)
    q_pack, k_pack = packs(q, k, wq, wk_ref[...].astype(bf16), dm)
    q_pack_ref[h] = q_pack
    k_pack_ref[h] = k_pack
    tokens = q_pack.shape[0]
    below = positions((tile, tile), 0) >= positions((tile, tile), 1)
    for i in range(tokens // tile):
        rows = slice(i * tile, (i + 1) * tile)
        numer = jnp.zeros((tile, v.shape[1]), f32)
        denom = jnp.zeros((tile, LANES), f32)
        for j in range(i + 1):
            cols = slice(j * tile, (j + 1) * tile)
            t = dot(q_pack[rows], k_pack[:, cols])
            weight = (0.5 * t) * t + 0.5
            if j == i:
                weight = jnp.where(below, weight, 0.0)
            for c in range(tile // LANES):
                denom = denom + weight[:, c * LANES : (c + 1) * LANES]
            numer = numer + dot(weight.astype(bf16), v[cols])
        numer_ref[h, rows, :] = numer
        denom_ref[h, rows, :] = denom


def feature_kernel(dm, per, p0, me_ref, q_ref, wq_ref, ext_ref, phi_ref, p1_ref, p2_ref, t_ref):
    h = pl.program_id(0)
    at = head_at(me_ref, per, p0 + h)
    wq = wq_ref[...].astype(bf16)
    side = sides(wq, dm)
    for cols in tiles(q_ref.shape[1]):
        phi = features_rows(q_ref[at, cols, :], side, dm)
        phi_ref[h, cols, :] = phi
        p1_ref[h, cols, :], p2_ref[h, cols, :] = split2(phi)
        t_ref[h, :, cols] = jnp.concatenate(split2(features_t(ext_ref[h, :, cols], dm)), 0)


def join_kernel(n, backward, me_ref, *refs):
    far, got, outs = refs[: -2 * n], refs[-2 * n : -n], refs[-n:]

    def before(a, b):
        return a > b if backward else a < b

    me, mine = me_ref[0], me_ref[1]
    outer = jnp.zeros(outs[0].shape, f32)
    for d, piece in enumerate(far, 1):
        outer = outer + jnp.where(before(mine ^ d, mine), piece[...], 0.0)
    for d, out in enumerate(outs):
        total = outer
        for e, piece in enumerate(got):
            if e != d:
                total = total + jnp.where(before(me ^ e, me ^ d), piece[...], 0.0)
        out[...] = total


def forward_kernel(dm, scale, per, p, i, me_ref, t_ref, *rest):
    used, slots, outs = rest[:6], rest[6 : 6 + per], rest[6 + per : 9 + per]
    backs, (scr,) = rest[9 + per : 9 + 2 * per], rest[9 + 2 * per :]
    state = get_slots(me_ref, slots, scr)
    teacher = t_ref.at[head_at(me_ref, per, p)]
    put_slots(me_ref, backs, scr, forward_head(dm, scale, state, teacher, *[ref.at[i] for ref in used], *outs))


def forward_head(
    dm, scale, state, teacher, numer_ref, denom_ref, phi_ref, p1_ref, p2_ref, phi_t_ref, student_ref, g_ref, gd_ref
):
    hd = state.shape[1]
    s_pack = jnp.concatenate(split2(state), 1)
    s_pack = jnp.concatenate([s_pack, jnp.zeros((dm.lanes - dm.rows, 2 * hd), bf16)], 0)
    before = count_of(state, dm)
    back, count = 0.0, 0.0
    for rows in tiles(teacher.shape[0]):
        phi = phi_ref[rows]
        prod = dot(p1_ref[rows], s_pack) + dot(p2_ref[rows], s_pack)
        numer = numer_ref[rows] + (prod[:, :hd] + prod[:, hd:])
        weighted = phi * before
        part = denom_ref[rows]
        for c in range(0, dm.lanes, LANES):
            part = part + weighted[:, c : c + LANES]
        inv = 1.0 / jnp.sum(part, 1, keepdims=True)
        y = numer * inv
        student_ref[rows] = y.astype(bf16)
        g_out = scale * (y - teacher[rows].astype(f32))
        g_numer = g_out * inv
        g_denom = -jnp.sum(g_out * y, 1, keepdims=True) * inv
        g_ref[rows] = g_numer
        gd_ref[rows] = jnp.broadcast_to(g_denom, part.shape)
        count = count + jnp.sum(phi * g_denom, 0, keepdims=True)
        back = back + dot(phi_t_ref[:, rows], jnp.concatenate(split2(g_numer), 1))
    back = back[: dm.rows] + back[dm.rows :]
    return with_count(back[:, :hd] + back[:, hd:], count, dm)


def count_column(state, dm):
    row, lane = positions((dm.rows, dm.lanes), 0), positions((dm.rows, dm.lanes), 1)
    return jnp.sum(jnp.where(row == lane, count_of(state, dm), 0.0), 1, keepdims=True)


def backward_kernel(dm, tile, per, p0, count, me_ref, q_ref, vt_ref, *rest):
    packed, rest = rest[:4], rest[4:]
    grads, rest = rest[: 2 * count], rest[2 * count :]
    slots, (gk_ref, wgrad_ref, scr) = rest[: per * count], rest[per * count :]
    grad = 0.0
    for i in range(count):
        state = get_slots(me_ref, slots[i * per : (i + 1) * per], scr)
        at = head_at(me_ref, per, p0 + i)
        refs = [ref.at[i] for ref in packed]
        gk_ref[i], head_grad = backward_head(dm, tile, state, q_ref.at[at], vt_ref.at[at], *grads[2 * i : 2 * i + 2], *refs)
        grad = grad + head_grad
    wgrad_ref[...] = grad


def backward_head(dm, tile, state, q, vt, g_numer, g_denom, q_pack, k_pack, q_two, ext):
    w = dm.width
    s_aug = jnp.concatenate(
        [state, jnp.where(positions((1, LANES), 1) == 0, count_column(state, dm), 0.0)], 1
    )
    s1, s2 = split2(s_aug)
    count = q_pack.shape[0] // tile
    below = positions((tile, tile), 0) >= positions((tile, tile), 1)
    g_q, g_k = [], 0.0
    for i in range(count):
        rows = slice(i * tile, (i + 1) * tile)
        width = (i + 1) * tile
        t = dot(q_pack[rows], k_pack[:, :width])
        g_weight = dot(g_numer[rows].astype(bf16), vt[:, :width]) + jnp.concatenate([g_denom[rows]] * (width // LANES), 1)
        score = g_weight * t
        last = jnp.where(below, score[:, width - tile :], 0.0)
        hi, lo = split2(jnp.concatenate([score[:, : width - tile], last], 1) if i else last)
        both = dot(k_pack[: 2 * w, :width], hi, NT)
        g_q.append(both[:w] + both[w:] + dot(k_pack[:w, :width], lo, NT))
        both = dot(q_two[:, rows], hi)
        part = both[:w] + both[w:] + dot(q_two[:w, rows], lo)
        rest = count * tile - width
        g_k = g_k + (jnp.concatenate([part, jnp.zeros((w, rest), f32)], 1) if rest else part)
    first = positions((1, LANES), 1) == 0
    a1, a2 = split2(jnp.concatenate([g_numer[...], jnp.where(first, g_denom[...], 0.0)], 1))
    both = dot(jnp.concatenate([s1, s2], 0), a1, NT)
    g_phi = both[: dm.rows] + both[dm.rows :] + dot(s1, a2, NT)
    total = jnp.concatenate(g_q, 1) + feature_grad_t(ext[...], g_phi, dm)
    return g_k, dot(total.astype(bf16), q[...])


def saving_kernel(body, per, n_in, heads, me_ref, *refs):
    used, pieces, outs = refs[: n_in - 1], refs[n_in - 1 : n_in - 1 + heads], refs[n_in - 1 + heads :]
    gk_ref, wgrad_ref, dst, scr, sems = outs
    copies = [
        pltpu.make_async_copy(piece, dst.at[head_at(me_ref, per, p)], sems.at[p]) for p, piece in enumerate(pieces)
    ]
    for copy in copies:
        copy.start()
    body(me_ref, *used, gk_ref, wgrad_ref, scr)
    for copy in copies:
        copy.wait()


def key_kernel(dm, n, parts, me_ref, k_ref, vt_ref, wk_ref, *rest):
    slots, backs, (out_ref, scr) = rest[:n], rest[n:-2], rest[-2:]
    per = n // k_ref.shape[0]
    w = dm.width
    out_ref[:w] = functools.reduce(jnp.add, [g[...] for g in backs[1::2]])
    w_ext = rolled(wk_ref[...].astype(bf16), dm)
    grad = jnp.zeros((w, out_ref.shape[1]), f32)
    for (p0, count), gk_ref in zip(parts, backs[::2]):
        for i in range(count):
            p = p0 + i
            state = get_slots(me_ref, slots[p * per : (p + 1) * per], scr)
            at = head_at(me_ref, per, p)
            k = k_ref[at]
            g_phi = dot(state.astype(bf16), vt_ref[at]) + count_column(state, dm)
            total = gk_ref[i] + feature_grad_t(dot(w_ext, k, NT), g_phi, dm)
            grad = grad + dot(total.astype(bf16), k)
    out_ref[w:] = grad


VMEM_LIMIT = 20 * 1024 * 1024
HBM = pl.BlockSpec(memory_space=pltpu.HBM)
VMEM = pl.BlockSpec(memory_space=pltpu.VMEM)
SMEM = pl.BlockSpec(memory_space=pltpu.SMEM)


def placed(args, specs):
    spaces = {id(HBM): pltpu.HBM, id(VMEM): pltpu.VMEM, id(SMEM): pltpu.SMEM}
    return [
        pltpu.with_memory_space_constraint(a, spaces[id(s)]) if id(s) in spaces else a
        for a, s in zip(args, specs)
    ]


def call(body, grid, args, specs, outs, out_specs, scratch, flops):
    return pl.pallas_call(
        body,
        grid=grid,
        in_specs=specs,
        out_specs=out_specs,
        out_shape=outs,
        scratch_shapes=scratch,
        compiler_params=pltpu.CompilerParams(
            dimension_semantics=("arbitrary",) * len(grid), vmem_limit_bytes=VMEM_LIMIT
        ),
        cost_estimate=pl.CostEstimate(flops=flops, bytes_accessed=0, transcendentals=0),
    )(*placed(args, specs))


def shifted(array, axis, pairs):
    return lax.ppermute(array, axis, pairs)


def exchange(parts, axis):
    n = lax.axis_size(axis)
    got = []
    for d, part in enumerate(parts):
        got.append(part if d == 0 else shifted(part, axis, [(i, i ^ d) for i in range(n)]))
    return got


def carried(me, parts, backward):
    n, m = lax.axis_size("seq"), lax.axis_size("seg")
    got = exchange(parts, "seq")
    total = functools.reduce(jnp.add, got)
    far = exchange([total] * m, "seg")[1:]
    shape = pltpu.VMEM(parts[0].shape, f32)
    before = call(
        functools.partial(join_kernel, n, backward),
        (),
        (me, *far, *got),
        [SMEM] + [VMEM] * (n + m - 1),
        [shape] * n,
        [VMEM] * n,
        [],
        parts[0].size * n * n,
    )
    return exchange(before, "seq")


def summed(array):
    for axis in ("head", "seq", "seg"):
        array = functools.reduce(jnp.add, exchange([array] * lax.axis_size(axis), axis))
    return array


SPLIT = (1, 2, 1)


def split_heads(heads, split):
    if heads % sum(split):
        return [(0, heads)]
    unit, at, out = heads // sum(split), 0, []
    for part in split:
        out.append((at, part * unit))
        at += part * unit
    return out


def shards(queries, keys, values, teacher, query_proj, key_proj):
    heads, tokens, hd = queries.shape
    dm = Dims(query_proj.shape[1])
    n = lax.axis_size("seq")
    assert n % heads == 0
    per = n // heads
    heads_all = heads * lax.axis_size("head")
    tokens_all = tokens * n * lax.axis_size("seg")
    scale = 1.0 / math.sqrt(heads_all * tokens_all)
    tile = min(256, tokens)
    wq, wk = query_proj.T, key_proj.T
    me = jnp.stack([lax.axis_index("seq"), lax.axis_index("seg")]).astype(jnp.int32)
    slot_shape = pltpu.VMEM((heads * dm.rows // n, hd), f32)
    grad_shape = pltpu.VMEM((dm.width, hd), f32)
    scr = [pltpu.VMEM((dm.rows, hd), f32)]

    sources = (wk, keys, values, wq)
    called = call(
        functools.partial(state_kernel, dm, n),
        (),
        (me, *sources),
        [SMEM] + [HBM] * len(sources),
        [slot_shape] * n + [pltpu.VMEM(a.shape, a.dtype) for a in sources] + [pltpu.SMEM((2,), jnp.int32)],
        [VMEM] * (n + len(sources)) + [SMEM],
        scr + [pltpu.SemaphoreType.DMA((len(sources),))],
        4 * heads * tokens * dm.rows * hd,
    )
    states, (wk, keys, values, wq, me) = called[:n], called[n:]
    vt, queries, teacher = call(
        turn_kernel,
        (),
        (values, queries, teacher),
        [VMEM, HBM, HBM],
        [pltpu.VMEM((heads, hd, tokens), bf16)] + [pltpu.VMEM(a.shape, bf16) for a in (queries, teacher)],
        [VMEM] * 3,
        [pltpu.SemaphoreType.DMA((2,))],
        heads * tokens * hd * hd,
    )
    intra, packed, parts = [], [], split_heads(heads, SPLIT)
    for p0, count in parts:
        outs = call(
            functools.partial(intra_kernel, dm, tile, per, p0),
            (count,),
            (me, queries, keys, values, wq, wk),
            [SMEM] + [VMEM] * 5,
            [
                pltpu.VMEM((count, tokens, hd), f32),
                pltpu.VMEM((count, tokens, LANES), f32),
                pltpu.VMEM((count, tokens, LANES), bf16),
                pltpu.VMEM((count, LANES, tokens), bf16),
                pltpu.VMEM((count, 2 * dm.width, tokens), bf16),
                pltpu.VMEM((count, dm.quad, tokens), f32),
            ],
            [VMEM] * 6,
            [],
            4 * count * tokens * tokens * hd,
        )
        outs += call(
            functools.partial(feature_kernel, dm, per, p0),
            (count,),
            (me, queries, wq, outs[5]),
            [SMEM] + [VMEM] * 3,
            [
                pltpu.VMEM((count, tokens, dm.lanes), f32),
                pltpu.VMEM((count, tokens, dm.lanes), bf16),
                pltpu.VMEM((count, tokens, dm.lanes), bf16),
                pltpu.VMEM((count, 2 * dm.rows, tokens), bf16),
            ],
            [VMEM] * 4,
            [],
            4 * count * tokens * dm.lanes * hd,
        )
        intra.append(outs[:2] + outs[6:])
        packed.append(outs[2:6])
    prev = carried(me, states, False)
    heads_out = {}
    for p, i, part in reversed([(p0 + i, i, part) for part, (p0, count) in enumerate(parts) for i in range(count)]):
        heads_out[p] = call(
            functools.partial(forward_kernel, dm, scale, per, p, i),
            (),
            (me, teacher, *intra[part], *prev[p * per : (p + 1) * per]),
            [SMEM] + [VMEM] * (7 + per),
            [
                pltpu.VMEM((tokens, hd), bf16),
                pltpu.VMEM((tokens, hd), f32),
                pltpu.VMEM((tokens, LANES), f32),
            ]
            + [slot_shape] * per,
            [VMEM] * (3 + per),
            scr,
            8 * tokens * dm.lanes * hd,
        )
    later = carried(me, [b for p in range(heads) for b in heads_out[p][3:]], True)
    backs = []
    for part, (p0, count) in enumerate(parts):
        body = functools.partial(backward_kernel, dm, tile, per, p0, count)
        args = (me, queries, vt, *packed[part])
        for i in range(count):
            args += tuple(heads_out[p0 + i][1:3])
        args += tuple(prev[p0 * per : (p0 + count) * per])
        outs = [pltpu.VMEM((count, dm.width, tokens), f32), grad_shape]
        specs, scratch = [VMEM] * len(outs), scr
        if part == 0:
            body = functools.partial(saving_kernel, body, per, len(args), heads)
            args += tuple(heads_out[p][0] for p in range(heads))
            outs, specs = outs + [pltpu.HBM((heads, tokens, hd), bf16)], specs + [HBM]
            scratch = scr + [pltpu.SemaphoreType.DMA((heads,))]
        outs = call(
            body, (), args, [SMEM] + [VMEM] * (len(args) - 1), outs, specs, scratch, 8 * count * tokens * tokens * hd
        )
        if part == 0:
            student = outs[2]
        backs += outs[:2]
    grads = call(
        functools.partial(key_kernel, dm, n, parts),
        (),
        (me, keys, vt, wk, *later, *backs),
        [SMEM] + [VMEM] * (3 + n + len(backs)),
        [pltpu.VMEM((2 * dm.width, hd), f32)],
        [VMEM],
        scr,
        4 * heads * tokens * dm.rows * hd,
    )[0]
    grads = summed(grads)
    return student, grads[: dm.width].T, grads[dm.width :].T


def solution(mesh):
    in_specs = (
        P("head", ("seg", "seq"), None),
        P("head", ("seg", "seq"), None),
        P("head", ("seg", "seq"), None),
        P("head", ("seg", "seq"), None),
        P(),
        P(),
    )
    out_specs = (P("head", ("seg", "seq"), None), P(), P())
    return jax.shard_map(shards, mesh=mesh, in_specs=in_specs, out_specs=out_specs, check_vma=False)
```

```python
import functools
import math

import jax
import jax.numpy as jnp
from jax import lax
from jax.experimental import pallas as pl
from jax.experimental.pallas import tpu as pltpu
from jax.sharding import PartitionSpec as P


f32 = jnp.float32
bf16 = jnp.bfloat16
HALF = 0.5**0.5
LANES = 128
NT = (((1,), (1,)), ((), ()))


class Dims:
    def __init__(self, width):
        self.width = width
        self.half = width // 2
        self.shift = width.bit_length() - 1
        assert width == 1 << self.shift
        self.quad = width * (width + 1) // 2
        self.lin = self.quad
        self.const = self.quad + width
        self.feats = self.const + 1
        self.lanes = -(-self.feats // LANES) * LANES
        self.count_rows = self.lanes // LANES
        self.rows = -(-(self.feats + self.count_rows) // 8) * 8


def positions(shape, dim):
    return lax.broadcasted_iota(jnp.int32, shape, dim)


def one_hot(hit):
    return jnp.where(hit, 1.0, 0.0).astype(bf16)


def first_of(dm, f):
    return jnp.where(f < dm.quad, f & (dm.width - 1), f - dm.lin)


def second_of(dm, f):
    return (f + (f >> dm.shift)) & (dm.width - 1)


def tiles(tokens, size=256):
    size = min(size, tokens)
    return [slice(i, i + size) for i in range(0, tokens, size)]


def dot(a, b, dims=(((1,), (0,)), ((), ()))):
    return lax.dot_general(a, b, dims, preferred_element_type=f32)


def split2(x):
    hi = x.astype(bf16)
    return hi, (x - hi.astype(f32)).astype(bf16)


def split3(x):
    hi = x.astype(bf16)
    rest = x - hi.astype(f32)
    mid = rest.astype(bf16)
    return hi, mid, (rest - mid.astype(f32)).astype(bf16)


def rolled(w_t, dm):
    shape = (dm.quad, dm.width)
    return dot(one_hot(second_of(dm, positions(shape, 0)) == positions(shape, 1)), w_t).astype(bf16)


def repeated(w_t, dm):
    shape = (LANES, dm.width)
    return dot(one_hot((positions(shape, 0) & (dm.width - 1)) == positions(shape, 1)), w_t).astype(bf16)


def sides(w_t, dm):
    shape = (dm.lanes, dm.width)
    f, j = positions(shape, 0), positions(shape, 1)
    left = dot(one_hot(first_of(dm, f) == j), w_t).astype(bf16)
    right = dot(one_hot((f < dm.quad) & (second_of(dm, f) == j)), w_t).astype(bf16)
    return left, right


def features_t(ext, dm):
    w = dm.width
    base = ext[:w]
    parts = [HALF * base * base]
    for d in range(1, dm.half):
        parts.append(ext[d * w : (d + 1) * w] * base)
    parts.append(ext[dm.half * w : dm.quad] * base[: dm.half])
    parts.append(base)
    tail = dm.rows - dm.const
    rows = lax.broadcasted_iota(jnp.int32, (tail, ext.shape[1]), 0)
    parts.append(jnp.where(rows == 0, 1.0, 0.0).astype(f32))
    return jnp.concatenate(parts, 0)


def features_rows(rows, side, dm):
    left, right = side
    f = positions((1, dm.lanes), 1)
    left = dot(rows, left, NT) + jnp.where(f == dm.const, 1.0, 0.0)
    right = dot(rows, right, NT) + jnp.where((f >= dm.lin) & (f < dm.feats), 1.0, 0.0)
    return jnp.where(f < dm.width, HALF, 1.0) * left * right


def feature_grad_t(ext, g, dm):
    w, half = dm.width, dm.half
    base = ext[:w]
    total = g[dm.lin : dm.lin + w] + (2.0 * HALF) * g[:w] * base
    for d in range(1, half):
        quad = g[d * w : (d + 1) * w]
        total = total + quad * ext[d * w : (d + 1) * w]
        back = quad * base
        total = total + jnp.concatenate([back[w - d :], back[: w - d]], 0)
    quad = g[half * w : dm.quad]
    return total + jnp.concatenate([quad * base[half:], quad * base[:half]], 0)


def with_count(state, count, dm):
    rows = lax.broadcasted_iota(jnp.int32, state.shape, 0)
    for c in range(dm.count_rows):
        state = jnp.where(rows == dm.feats + c, count[:, c * LANES : (c + 1) * LANES], state)
    return state


def count_of(state, dm):
    return jnp.concatenate([state[dm.feats + c : dm.feats + c + 1] for c in range(dm.count_rows)], 1)


def column_row(part, dm):
    column = jnp.sum(part, 1, keepdims=True)
    row, lane = positions((dm.rows, dm.lanes), 0), positions((dm.rows, dm.lanes), 1)
    return jnp.sum(jnp.where(row == lane, column, 0.0), 0, keepdims=True)


def head_at(me_ref, per, p):
    return (me_ref[0] >> (per.bit_length() - 1)) ^ p


def put_slots(me_ref, slots, scr, value):
    if len(slots) == 1:
        slots[0][...] = value
        return
    scr[...] = value
    size = slots[0].shape[0]
    for c, slot in enumerate(slots):
        slot[...] = scr[pl.ds(pl.multiple_of(((me_ref[0] & (len(slots) - 1)) ^ c) * size, 8), size), :]


def get_slots(me_ref, slots, scr):
    if len(slots) == 1:
        return slots[0][...]
    size = slots[0].shape[0]
    for c, slot in enumerate(slots):
        scr[pl.ds(pl.multiple_of(((me_ref[0] & (len(slots) - 1)) ^ c) * size, 8), size), :] = slot[...]
    return scr[...]


def state_kernel(dm, n, me_ref, *rest):
    sources, slots, kept, at_ref, scr, sems = rest[:4], rest[4 : 4 + n], rest[4 + n : 8 + n], *rest[8 + n :]
    at_ref[0] = me_ref[0]
    at_ref[1] = me_ref[1]
    wk_ref, k_ref, v_ref = kept[:3]
    heads = k_ref.shape[0]
    per = n // heads
    whole = [pltpu.make_async_copy(a, b, sems.at[i]) for i, (a, b) in enumerate(zip(sources, kept)) if i in (0, 3)]

    def one(i, p):
        at = head_at(me_ref, per, p)
        return pltpu.make_async_copy(sources[i].at[at], kept[i].at[at], sems.at[4 + 2 * p + i - 1])

    whole[0].start()
    for i in (1, 2):
        for p in range(heads):
            one(i, p).start()
    whole[1].start()
    whole[0].wait()
    w_ext = rolled(wk_ref[...].astype(bf16), dm)
    for p in range(heads):
        one(1, p).wait()
    phis, parts = [], []
    for p in range(heads):
        phi = features_t(dot(w_ext, k_ref[head_at(me_ref, per, p)], NT), dm)
        part = phi[:, :LANES]
        for c in range(LANES, phi.shape[1], LANES):
            part = part + phi[:, c : c + LANES]
        phis.append(phi.astype(bf16))
        parts.append(part)
    for p in range(heads):
        one(2, p).wait()
    whole[1].wait()
    for p in range(heads):
        state = with_count(dot(phis[p], v_ref[head_at(me_ref, per, p)]), column_row(parts[p], dm), dm)
        put_slots(me_ref, slots[p * per : (p + 1) * per], scr, state)


def turn_kernel(v_ref, q_hbm, t_hbm, vt_ref, q_ref, t_ref, sems):
    copies = [pltpu.make_async_copy(a, b, sems.at[i]) for i, (a, b) in enumerate(((q_hbm, q_ref), (t_hbm, t_ref)))]
    for copy in copies:
        copy.start()
    for h in range(v_ref.shape[0]):
        vt_ref[h] = v_ref[h].T
    for copy in copies:
        copy.wait()


def packs(q, k, wq, wk, dm):
    w = dm.width
    q1, q2, q3 = split3(dot(q, repeated(wq, dm), NT))
    group = positions((1, LANES), 1)
    zero = jnp.zeros((), bf16)

    def at(lo, hi):
        return (group >= lo * w) & (group < hi * w)

    q_pack = jnp.where(at(0, 3), q1, jnp.where(at(3, 5), q2, jnp.where(at(5, 6), q3, zero)))
    q_pack = jnp.where(group == 6 * w, jnp.ones((), bf16), q_pack)
    k_t = dot(wk, k, NT)
    k1, k2, k3 = split3(k_t)
    last = one_hot(positions((LANES - 6 * w, k_t.shape[1]), 0) == 0)
    return q_pack, jnp.concatenate([k1, k2, k3, k1, k2, k1, last], 0)


def intra_kernel(dm, tile, per, p0, me_ref, q_ref, k_ref, v_ref, wq_ref, wk_ref, *outs):
    numer_ref, denom_ref, q_pack_ref, k_pack_ref, q_two_ref, ext_ref = outs
    h = pl.program_id(0)
    at = head_at(me_ref, per, p0 + h)
    q, k, v = q_ref[at], k_ref[at], v_ref.at[at]
    wq = wq_ref[...].astype(bf16)
    ext = dot(rolled(wq, dm), q, NT)
    ext_ref[h] = ext
    q_two_ref[h] = jnp.concatenate(split2(ext[: dm.width]), 0)
    q_pack, k_pack = packs(q, k, wq, wk_ref[...].astype(bf16), dm)
    q_pack_ref[h] = q_pack
    k_pack_ref[h] = k_pack
    tokens = q_pack.shape[0]
    below = positions((tile, tile), 0) >= positions((tile, tile), 1)
    for i in range(tokens // tile):
        rows = slice(i * tile, (i + 1) * tile)
        numer = jnp.zeros((tile, v.shape[1]), f32)
        denom = jnp.zeros((tile, LANES), f32)
        for j in range(i + 1):
            cols = slice(j * tile, (j + 1) * tile)
            t = dot(q_pack[rows], k_pack[:, cols])
            weight = (0.5 * t) * t + 0.5
            if j == i:
                weight = jnp.where(below, weight, 0.0)
            for c in range(tile // LANES):
                denom = denom + weight[:, c * LANES : (c + 1) * LANES]
            numer = numer + dot(weight.astype(bf16), v[cols])
        numer_ref[h, rows, :] = numer
        denom_ref[h, rows, :] = denom


def feature_kernel(dm, per, p0, me_ref, q_ref, wq_ref, ext_ref, phi_ref, p1_ref, p2_ref, t_ref):
    h = pl.program_id(0)
    at = head_at(me_ref, per, p0 + h)
    wq = wq_ref[...].astype(bf16)
    side = sides(wq, dm)
    for cols in tiles(q_ref.shape[1]):
        phi = features_rows(q_ref[at, cols, :], side, dm)
        phi_ref[h, cols, :] = phi
        p1_ref[h, cols, :], p2_ref[h, cols, :] = split2(phi)
        t_ref[h, :, cols] = jnp.concatenate(split2(features_t(ext_ref[h, :, cols], dm)), 0)


def join_kernel(n, backward, me_ref, *refs):
    far, got, outs = refs[: -2 * n], refs[-2 * n : -n], refs[-n:]

    def before(a, b):
        return a > b if backward else a < b

    me, mine = me_ref[0], me_ref[1]
    outer = jnp.zeros(outs[0].shape, f32)
    for d, piece in enumerate(far, 1):
        outer = outer + jnp.where(before(mine ^ d, mine), piece[...], 0.0)
    for d, out in enumerate(outs):
        total = outer
        for e, piece in enumerate(got):
            if e != d:
                total = total + jnp.where(before(me ^ e, me ^ d), piece[...], 0.0)
        out[...] = total


def forward_kernel(dm, scale, per, p, i, me_ref, t_ref, *rest):
    used, slots, outs = rest[:6], rest[6 : 6 + per], rest[6 + per : 9 + per]
    backs, (scr,) = rest[9 + per : 9 + 2 * per], rest[9 + 2 * per :]
    state = get_slots(me_ref, slots, scr)
    teacher = t_ref.at[head_at(me_ref, per, p)]
    put_slots(me_ref, backs, scr, forward_head(dm, scale, state, teacher, *[ref.at[i] for ref in used], *outs))


def forward_head(
    dm, scale, state, teacher, numer_ref, denom_ref, phi_ref, p1_ref, p2_ref, phi_t_ref, student_ref, g_ref, gd_ref
):
    hd = state.shape[1]
    s_pack = jnp.concatenate(split2(state), 1)
    s_pack = jnp.concatenate([s_pack, jnp.zeros((dm.lanes - dm.rows, 2 * hd), bf16)], 0)
    before = count_of(state, dm)
    back, count = 0.0, 0.0
    for rows in tiles(teacher.shape[0]):
        phi = phi_ref[rows]
        prod = dot(p1_ref[rows], s_pack) + dot(p2_ref[rows], s_pack)
        numer = numer_ref[rows] + (prod[:, :hd] + prod[:, hd:])
        weighted = phi * before
        part = denom_ref[rows]
        for c in range(0, dm.lanes, LANES):
            part = part + weighted[:, c : c + LANES]
        inv = 1.0 / jnp.sum(part, 1, keepdims=True)
        y = numer * inv
        student_ref[rows] = y.astype(bf16)
        g_out = scale * (y - teacher[rows].astype(f32))
        g_numer = g_out * inv
        g_denom = -jnp.sum(g_out * y, 1, keepdims=True) * inv
        g_ref[rows] = g_numer
        gd_ref[rows] = jnp.broadcast_to(g_denom, part.shape)
        count = count + jnp.sum(phi * g_denom, 0, keepdims=True)
        back = back + dot(phi_t_ref[:, rows], jnp.concatenate(split2(g_numer), 1))
    back = back[: dm.rows] + back[dm.rows :]
    return with_count(back[:, :hd] + back[:, hd:], count, dm)


def count_column(state, dm):
    row, lane = positions((dm.rows, dm.lanes), 0), positions((dm.rows, dm.lanes), 1)
    return jnp.sum(jnp.where(row == lane, count_of(state, dm), 0.0), 1, keepdims=True)


def backward_kernel(dm, tile, per, p0, count, me_ref, q_ref, vt_ref, *rest):
    packed, rest = rest[:4], rest[4:]
    grads, rest = rest[: 2 * count], rest[2 * count :]
    slots, (gk_ref, wgrad_ref, scr) = rest[: per * count], rest[per * count :]
    grad = 0.0
    for i in range(count):
        state = get_slots(me_ref, slots[i * per : (i + 1) * per], scr)
        at = head_at(me_ref, per, p0 + i)
        refs = [ref.at[i] for ref in packed]
        gk_ref[i], head_grad = backward_head(dm, tile, state, q_ref.at[at], vt_ref.at[at], *grads[2 * i : 2 * i + 2], *refs)
        grad = grad + head_grad
    wgrad_ref[...] = grad


def backward_head(dm, tile, state, q, vt, g_numer, g_denom, q_pack, k_pack, q_two, ext):
    w = dm.width
    s_aug = jnp.concatenate(
        [state, jnp.where(positions((1, LANES), 1) == 0, count_column(state, dm), 0.0)], 1
    )
    s1, s2 = split2(s_aug)
    count = q_pack.shape[0] // tile
    below = positions((tile, tile), 0) >= positions((tile, tile), 1)
    g_q, g_k = [], 0.0
    for i in range(count):
        rows = slice(i * tile, (i + 1) * tile)
        width = (i + 1) * tile
        t = dot(q_pack[rows], k_pack[:, :width])
        g_weight = dot(g_numer[rows].astype(bf16), vt[:, :width]) + jnp.concatenate([g_denom[rows]] * (width // LANES), 1)
        score = g_weight * t
        last = jnp.where(below, score[:, width - tile :], 0.0)
        hi, lo = split2(jnp.concatenate([score[:, : width - tile], last], 1) if i else last)
        both = dot(k_pack[: 2 * w, :width], hi, NT)
        g_q.append(both[:w] + both[w:] + dot(k_pack[:w, :width], lo, NT))
        both = dot(q_two[:, rows], hi)
        part = both[:w] + both[w:] + dot(q_two[:w, rows], lo)
        rest = count * tile - width
        g_k = g_k + (jnp.concatenate([part, jnp.zeros((w, rest), f32)], 1) if rest else part)
    first = positions((1, LANES), 1) == 0
    a1, a2 = split2(jnp.concatenate([g_numer[...], jnp.where(first, g_denom[...], 0.0)], 1))
    both = dot(jnp.concatenate([s1, s2], 0), a1, NT)
    g_phi = both[: dm.rows] + both[dm.rows :] + dot(s1, a2, NT)
    total = jnp.concatenate(g_q, 1) + feature_grad_t(ext[...], g_phi, dm)
    return g_k, dot(total.astype(bf16), q[...])


def saving_kernel(body, per, n_in, heads, me_ref, *refs):
    used, pieces, outs = refs[: n_in - 1], refs[n_in - 1 : n_in - 1 + heads], refs[n_in - 1 + heads :]
    gk_ref, wgrad_ref, dst, scr, sems = outs
    copies = [
        pltpu.make_async_copy(piece, dst.at[head_at(me_ref, per, p)], sems.at[p]) for p, piece in enumerate(pieces)
    ]
    for copy in copies:
        copy.start()
    body(me_ref, *used, gk_ref, wgrad_ref, scr)
    for copy in copies:
        copy.wait()


def key_kernel(dm, per, places, first, me_ref, k_ref, vt_ref, wk_ref, *rest):
    count = len(places)
    slots, backs = rest[: per * count], rest[per * count : (per + 1) * count]
    before, (out_ref, scr) = rest[(per + 1) * count : -2], rest[-2:]
    w = dm.width
    w_ext = rolled(wk_ref[...].astype(bf16), dm)
    grad = jnp.zeros((w, out_ref.shape[1]), f32) if first else before[0][w:]
    for at, ((p, i), gk_ref) in enumerate(zip(places, backs)):
        state = get_slots(me_ref, slots[at * per : (at + 1) * per], scr)
        h = head_at(me_ref, per, p)
        k = k_ref[h]
        g_phi = dot(state.astype(bf16), vt_ref[h]) + count_column(state, dm)
        total = gk_ref[i] + feature_grad_t(dot(w_ext, k, NT), g_phi, dm)
        grad = grad + dot(total.astype(bf16), k)
    out_ref[:w] = functools.reduce(jnp.add, [g[...] for g in before]) if first else before[0][:w]
    out_ref[w:] = grad


VMEM_LIMIT = 20 * 1024 * 1024
HBM = pl.BlockSpec(memory_space=pltpu.HBM)
VMEM = pl.BlockSpec(memory_space=pltpu.VMEM)
SMEM = pl.BlockSpec(memory_space=pltpu.SMEM)


def placed(args, specs):
    spaces = {id(HBM): pltpu.HBM, id(VMEM): pltpu.VMEM, id(SMEM): pltpu.SMEM}
    return [
        pltpu.with_memory_space_constraint(a, spaces[id(s)]) if id(s) in spaces else a
        for a, s in zip(args, specs)
    ]


def call(body, grid, args, specs, outs, out_specs, scratch, flops):
    return pl.pallas_call(
        body,
        grid=grid,
        in_specs=specs,
        out_specs=out_specs,
        out_shape=outs,
        scratch_shapes=scratch,
        compiler_params=pltpu.CompilerParams(
            dimension_semantics=("arbitrary",) * len(grid), vmem_limit_bytes=VMEM_LIMIT
        ),
        cost_estimate=pl.CostEstimate(flops=flops, bytes_accessed=0, transcendentals=0),
    )(*placed(args, specs))


def shifted(array, axis, pairs):
    return lax.ppermute(array, axis, pairs)


def crossed(array, axis, d):
    n, h = lax.axis_size(axis), lax.axis_size("head")
    return shifted(array, (axis, "head"), [(i * h + c, (i ^ d) * h + h - 1 - c) for i in range(n) for c in range(h)])


def exchange(parts, axis, cross=False):
    n = lax.axis_size(axis)
    got = []
    for d, part in enumerate(parts):
        if cross:
            got.append(crossed(part, axis, d))
        else:
            got.append(part if d == 0 else shifted(part, axis, [(i, i ^ d) for i in range(n)]))
    return got


def carried(me, parts, backward, label):
    n, m = lax.axis_size("seq"), lax.axis_size("seg")
    cross = label in CROSSED and lax.axis_size("head") > 1
    got = exchange(parts, "seq", cross)
    total = functools.reduce(jnp.add, got)
    far = exchange([total] * m, "seg")[1:]
    shape = pltpu.VMEM(parts[0].shape, f32)
    before = call(
        functools.partial(join_kernel, n, backward),
        (),
        (me, *far, *got),
        [SMEM] + [VMEM] * (n + m - 1),
        [shape] * n,
        [VMEM] * n,
        [],
        parts[0].size * n * n,
    )
    return exchange(before, "seq", cross)


def summed(array):
    array = functools.reduce(jnp.add, exchange([array] * lax.axis_size("head"), "head"))
    for axis in ("seq", "seg"):
        got = array
        for d in range(1, lax.axis_size(axis)):
            got = got + crossed(array, axis, d)
        array = got
    return array


SPLIT = (1, 2, 1)
CROSSED = ("f",)


def split_heads(heads, split):
    if heads % sum(split):
        return [(0, heads)]
    unit, at, out = heads // sum(split), 0, []
    for part in split:
        out.append((at, part * unit))
        at += part * unit
    return out


def shards(queries, keys, values, teacher, query_proj, key_proj):
    heads, tokens, hd = queries.shape
    dm = Dims(query_proj.shape[1])
    n = lax.axis_size("seq")
    assert n % heads == 0
    per = n // heads
    heads_all = heads * lax.axis_size("head")
    tokens_all = tokens * n * lax.axis_size("seg")
    scale = 1.0 / math.sqrt(heads_all * tokens_all)
    tile = min(256, tokens)
    wq, wk = query_proj.T, key_proj.T
    me = jnp.stack([lax.axis_index("seq"), lax.axis_index("seg")]).astype(jnp.int32)
    slot_shape = pltpu.VMEM((heads * dm.rows // n, hd), f32)
    grad_shape = pltpu.VMEM((dm.width, hd), f32)
    scr = [pltpu.VMEM((dm.rows, hd), f32)]

    sources = (wk, keys, values, wq)
    called = call(
        functools.partial(state_kernel, dm, n),
        (),
        (me, *sources),
        [SMEM] + [HBM] * len(sources),
        [slot_shape] * n + [pltpu.VMEM(a.shape, a.dtype) for a in sources] + [pltpu.SMEM((2,), jnp.int32)],
        [VMEM] * (n + len(sources)) + [SMEM],
        scr + [pltpu.SemaphoreType.DMA((4 + 2 * heads,))],
        4 * heads * tokens * dm.rows * hd,
    )
    states, (wk, keys, values, wq, me) = called[:n], called[n:]
    vt, queries, teacher = call(
        turn_kernel,
        (),
        (values, queries, teacher),
        [VMEM, HBM, HBM],
        [pltpu.VMEM((heads, hd, tokens), bf16)] + [pltpu.VMEM(a.shape, bf16) for a in (queries, teacher)],
        [VMEM] * 3,
        [pltpu.SemaphoreType.DMA((2,))],
        heads * tokens * hd * hd,
    )
    intra, packed, parts = [], [], split_heads(heads, SPLIT)
    for p0, count in parts:
        outs = call(
            functools.partial(intra_kernel, dm, tile, per, p0),
            (count,),
            (me, queries, keys, values, wq, wk),
            [SMEM] + [VMEM] * 5,
            [
                pltpu.VMEM((count, tokens, hd), f32),
                pltpu.VMEM((count, tokens, LANES), f32),
                pltpu.VMEM((count, tokens, LANES), bf16),
                pltpu.VMEM((count, LANES, tokens), bf16),
                pltpu.VMEM((count, 2 * dm.width, tokens), bf16),
                pltpu.VMEM((count, dm.quad, tokens), f32),
            ],
            [VMEM] * 6,
            [],
            4 * count * tokens * tokens * hd,
        )
        outs += call(
            functools.partial(feature_kernel, dm, per, p0),
            (count,),
            (me, queries, wq, outs[5]),
            [SMEM] + [VMEM] * 3,
            [
                pltpu.VMEM((count, tokens, dm.lanes), f32),
                pltpu.VMEM((count, tokens, dm.lanes), bf16),
                pltpu.VMEM((count, tokens, dm.lanes), bf16),
                pltpu.VMEM((count, 2 * dm.rows, tokens), bf16),
            ],
            [VMEM] * 4,
            [],
            4 * count * tokens * dm.lanes * hd,
        )
        intra.append(outs[:2] + outs[6:])
        packed.append(outs[2:6])
    prev = carried(me, states, False, "f")
    heads_out = {}
    for p, i, part in reversed([(p0 + i, i, part) for part, (p0, count) in enumerate(parts) for i in range(count)]):
        heads_out[p] = call(
            functools.partial(forward_kernel, dm, scale, per, p, i),
            (),
            (me, teacher, *intra[part], *prev[p * per : (p + 1) * per]),
            [SMEM] + [VMEM] * (7 + per),
            [
                pltpu.VMEM((tokens, hd), bf16),
                pltpu.VMEM((tokens, hd), f32),
                pltpu.VMEM((tokens, LANES), f32),
            ]
            + [slot_shape] * per,
            [VMEM] * (3 + per),
            scr,
            8 * tokens * dm.lanes * hd,
        )
    later = carried(me, [b for p in range(heads) for b in heads_out[p][3:]], True, "b")
    backs = []
    for part, (p0, count) in enumerate(parts):
        body = functools.partial(backward_kernel, dm, tile, per, p0, count)
        args = (me, queries, vt, *packed[part])
        for i in range(count):
            args += tuple(heads_out[p0 + i][1:3])
        args += tuple(prev[p0 * per : (p0 + count) * per])
        outs = [pltpu.VMEM((count, dm.width, tokens), f32), grad_shape]
        specs, scratch = [VMEM] * len(outs), scr
        if part == 0:
            body = functools.partial(saving_kernel, body, per, len(args), heads)
            args += tuple(heads_out[p][0] for p in range(heads))
            outs, specs = outs + [pltpu.HBM((heads, tokens, hd), bf16)], specs + [HBM]
            scratch = scr + [pltpu.SemaphoreType.DMA((heads,))]
        outs = call(
            body, (), args, [SMEM] + [VMEM] * (len(args) - 1), outs, specs, scratch, 8 * count * tokens * tokens * hd
        )
        if part == 0:
            student = outs[2]
        backs += outs[:2]
    spots = [(p0 + i, i, part) for part, (p0, count) in enumerate(parts) for i in range(count)]
    grads = backs[1::2]
    for step, group in enumerate((spots[:1], spots[1:])):
        args = (me, keys, vt, wk)
        for p, _, _ in group:
            args += tuple(later[p * per : (p + 1) * per])
        args += tuple(backs[2 * part] for _, _, part in group) + tuple(grads)
        grads = call(
            functools.partial(key_kernel, dm, per, [(p, i) for p, i, _ in group], step == 0),
            (),
            args,
            [SMEM] + [VMEM] * (len(args) - 1),
            [pltpu.VMEM((2 * dm.width, hd), f32)],
            [VMEM],
            scr,
            4 * len(group) * tokens * dm.rows * hd,
        )
    (grads,) = grads
    grads = summed(grads)
    return student, grads[: dm.width].T, grads[dm.width :].T


def solution(mesh):
    in_specs = (
        P("head", ("seg", "seq"), None),
        P("head", ("seg", "seq"), None),
        P("head", ("seg", "seq"), None),
        P("head", ("seg", "seq"), None),
        P(),
        P(),
    )
    out_specs = (P("head", ("seg", "seq"), None), P(), P())
    return jax.shard_map(shards, mesh=mesh, in_specs=in_specs, out_specs=out_specs, check_vma=False)
```

```python
import functools
import math

import jax
import jax.numpy as jnp
from jax import lax
from jax.experimental import pallas as pl
from jax.experimental.pallas import tpu as pltpu
from jax.sharding import PartitionSpec as P


f32 = jnp.float32
bf16 = jnp.bfloat16
HALF = 0.5**0.5
LANES = 128
NT = (((1,), (1,)), ((), ()))


class Dims:
    def __init__(self, width):
        self.width = width
        self.half = width // 2
        self.shift = width.bit_length() - 1
        assert width == 1 << self.shift
        self.quad = width * (width + 1) // 2
        self.lin = self.quad
        self.const = self.quad + width
        self.feats = self.const + 1
        self.lanes = -(-self.feats // LANES) * LANES
        self.count_rows = self.lanes // LANES
        self.rows = -(-(self.feats + self.count_rows) // 8) * 8


def positions(shape, dim):
    return lax.broadcasted_iota(jnp.int32, shape, dim)


def one_hot(hit):
    return jnp.where(hit, 1.0, 0.0).astype(bf16)


def first_of(dm, f):
    return jnp.where(f < dm.quad, f & (dm.width - 1), f - dm.lin)


def second_of(dm, f):
    return (f + (f >> dm.shift)) & (dm.width - 1)


def tiles(tokens, size=256):
    size = min(size, tokens)
    return [slice(i, i + size) for i in range(0, tokens, size)]


def dot(a, b, dims=(((1,), (0,)), ((), ()))):
    return lax.dot_general(a, b, dims, preferred_element_type=f32)


def split2(x):
    hi = x.astype(bf16)
    return hi, (x - hi.astype(f32)).astype(bf16)


def split3(x):
    hi = x.astype(bf16)
    rest = x - hi.astype(f32)
    mid = rest.astype(bf16)
    return hi, mid, (rest - mid.astype(f32)).astype(bf16)


def rolled(w_t, dm):
    shape = (dm.quad, dm.width)
    return dot(one_hot(second_of(dm, positions(shape, 0)) == positions(shape, 1)), w_t).astype(bf16)


def repeated(w_t, dm):
    shape = (LANES, dm.width)
    return dot(one_hot((positions(shape, 0) & (dm.width - 1)) == positions(shape, 1)), w_t).astype(bf16)


def sides(w_t, dm):
    shape = (dm.lanes, dm.width)
    f, j = positions(shape, 0), positions(shape, 1)
    left = dot(one_hot(first_of(dm, f) == j), w_t).astype(bf16)
    right = dot(one_hot((f < dm.quad) & (second_of(dm, f) == j)), w_t).astype(bf16)
    return left, right


def features_t(ext, dm):
    w = dm.width
    base = ext[:w]
    parts = [HALF * base * base]
    for d in range(1, dm.half):
        parts.append(ext[d * w : (d + 1) * w] * base)
    parts.append(ext[dm.half * w : dm.quad] * base[: dm.half])
    parts.append(base)
    tail = dm.rows - dm.const
    rows = lax.broadcasted_iota(jnp.int32, (tail, ext.shape[1]), 0)
    parts.append(jnp.where(rows == 0, 1.0, 0.0).astype(f32))
    return jnp.concatenate(parts, 0)


def features_rows(rows, side, dm):
    left, right = side
    f = positions((1, dm.lanes), 1)
    left = dot(rows, left, NT) + jnp.where(f == dm.const, 1.0, 0.0)
    right = dot(rows, right, NT) + jnp.where((f >= dm.lin) & (f < dm.feats), 1.0, 0.0)
    return jnp.where(f < dm.width, HALF, 1.0) * left * right


def feature_grad_t(ext, g, dm):
    w, half = dm.width, dm.half
    base = ext[:w]
    total = g[dm.lin : dm.lin + w] + (2.0 * HALF) * g[:w] * base
    for d in range(1, half):
        quad = g[d * w : (d + 1) * w]
        total = total + quad * ext[d * w : (d + 1) * w]
        back = quad * base
        total = total + jnp.concatenate([back[w - d :], back[: w - d]], 0)
    quad = g[half * w : dm.quad]
    return total + jnp.concatenate([quad * base[half:], quad * base[:half]], 0)


def with_count(state, count, dm):
    rows = lax.broadcasted_iota(jnp.int32, state.shape, 0)
    for c in range(dm.count_rows):
        state = jnp.where(rows == dm.feats + c, count[:, c * LANES : (c + 1) * LANES], state)
    return state


def count_of(state, dm):
    return jnp.concatenate([state[dm.feats + c : dm.feats + c + 1] for c in range(dm.count_rows)], 1)


def column_row(part, dm):
    column = jnp.sum(part, 1, keepdims=True)
    row, lane = positions((dm.rows, dm.lanes), 0), positions((dm.rows, dm.lanes), 1)
    return jnp.sum(jnp.where(row == lane, column, 0.0), 0, keepdims=True)


def head_at(me_ref, per, p):
    return (me_ref[0] >> (per.bit_length() - 1)) ^ p


def put_slots(me_ref, slots, scr, value):
    if len(slots) == 1:
        slots[0][...] = value
        return
    scr[...] = value
    size = slots[0].shape[0]
    for c, slot in enumerate(slots):
        slot[...] = scr[pl.ds(pl.multiple_of(((me_ref[0] & (len(slots) - 1)) ^ c) * size, 8), size), :]


def get_slots(me_ref, slots, scr):
    if len(slots) == 1:
        return slots[0][...]
    size = slots[0].shape[0]
    for c, slot in enumerate(slots):
        scr[pl.ds(pl.multiple_of(((me_ref[0] & (len(slots) - 1)) ^ c) * size, 8), size), :] = slot[...]
    return scr[...]


def state_kernel(dm, n, me_ref, *rest):
    sources, slots, kept, at_ref, scr, sems = rest[:4], rest[4 : 4 + n], rest[4 + n : 8 + n], *rest[8 + n :]
    at_ref[0] = me_ref[0]
    at_ref[1] = me_ref[1]
    wk_ref, k_ref, v_ref = kept[:3]
    heads = k_ref.shape[0]
    per = n // heads
    whole = [pltpu.make_async_copy(a, b, sems.at[i]) for i, (a, b) in enumerate(zip(sources, kept)) if i in (0, 3)]

    def one(i, p):
        at = head_at(me_ref, per, p)
        return pltpu.make_async_copy(sources[i].at[at], kept[i].at[at], sems.at[4 + 2 * p + i - 1])

    whole[0].start()
    for i in (1, 2):
        for p in range(heads):
            one(i, p).start()
    whole[1].start()
    whole[0].wait()
    w_ext = rolled(wk_ref[...].astype(bf16), dm)
    for p in range(heads):
        one(1, p).wait()
    phis, parts = [], []
    for p in range(heads):
        phi = features_t(dot(w_ext, k_ref[head_at(me_ref, per, p)], NT), dm)
        part = phi[:, :LANES]
        for c in range(LANES, phi.shape[1], LANES):
            part = part + phi[:, c : c + LANES]
        phis.append(phi.astype(bf16))
        parts.append(part)
    for p in range(heads):
        one(2, p).wait()
    whole[1].wait()
    for p in range(heads):
        state = with_count(dot(phis[p], v_ref[head_at(me_ref, per, p)]), column_row(parts[p], dm), dm)
        put_slots(me_ref, slots[p * per : (p + 1) * per], scr, state)


def turn_kernel(v_ref, q_hbm, t_hbm, vt_ref, q_ref, t_ref, sems):
    copies = [pltpu.make_async_copy(a, b, sems.at[i]) for i, (a, b) in enumerate(((q_hbm, q_ref), (t_hbm, t_ref)))]
    for copy in copies:
        copy.start()
    for h in range(v_ref.shape[0]):
        vt_ref[h] = v_ref[h].T
    for copy in copies:
        copy.wait()


def packs(q, k, wq, wk, dm):
    w = dm.width
    q1, q2, q3 = split3(dot(q, repeated(wq, dm), NT))
    group = positions((1, LANES), 1)
    zero = jnp.zeros((), bf16)

    def at(lo, hi):
        return (group >= lo * w) & (group < hi * w)

    q_pack = jnp.where(at(0, 3), q1, jnp.where(at(3, 5), q2, jnp.where(at(5, 6), q3, zero)))
    q_pack = jnp.where(group == 6 * w, jnp.ones((), bf16), q_pack)
    k_t = dot(wk, k, NT)
    k1, k2, k3 = split3(k_t)
    last = one_hot(positions((LANES - 6 * w, k_t.shape[1]), 0) == 0)
    return q_pack, jnp.concatenate([k1, k2, k3, k1, k2, k1, last], 0)


def intra_kernel(dm, tile, per, p0, me_ref, q_ref, k_ref, v_ref, wq_ref, wk_ref, *outs):
    numer_ref, denom_ref, q_pack_ref, k_pack_ref, q_two_ref, ext_ref = outs
    h = pl.program_id(0)
    at = head_at(me_ref, per, p0 + h)
    q, k, v = q_ref[at], k_ref[at], v_ref.at[at]
    wq = wq_ref[...].astype(bf16)
    ext = dot(rolled(wq, dm), q, NT)
    ext_ref[h] = ext
    q_two_ref[h] = jnp.concatenate(split2(ext[: dm.width]), 0)
    q_pack, k_pack = packs(q, k, wq, wk_ref[...].astype(bf16), dm)
    q_pack_ref[h] = q_pack
    k_pack_ref[h] = k_pack
    tokens = q_pack.shape[0]
    below = positions((tile, tile), 0) >= positions((tile, tile), 1)
    for i in range(tokens // tile):
        rows = slice(i * tile, (i + 1) * tile)
        width = (i + 1) * tile
        t = dot(q_pack[rows], k_pack[:, :width])
        weight = (0.5 * t) * t + 0.5
        last = jnp.where(below, weight[:, width - tile :], 0.0)
        weight = jnp.concatenate([weight[:, : width - tile], last], 1) if i else last
        numer_ref[h, rows, :] = dot(weight.astype(bf16), v[:width])
        denom = weight[:, :LANES]
        for c in range(LANES, width, LANES):
            denom = denom + weight[:, c : c + LANES]
        denom_ref[h, rows, :] = denom


def feature_kernel(dm, per, p0, me_ref, q_ref, wq_ref, ext_ref, phi_ref, p1_ref, p2_ref, t_ref):
    h = pl.program_id(0)
    at = head_at(me_ref, per, p0 + h)
    wq = wq_ref[...].astype(bf16)
    side = sides(wq, dm)
    for cols in tiles(q_ref.shape[1]):
        phi = features_rows(q_ref[at, cols, :], side, dm)
        phi_ref[h, cols, :] = phi
        p1_ref[h, cols, :], p2_ref[h, cols, :] = split2(phi)
        t_ref[h, :, cols] = jnp.concatenate(split2(features_t(ext_ref[h, :, cols], dm)), 0)


def join_kernel(n, backward, me_ref, *refs):
    far, got, outs = refs[: -2 * n], refs[-2 * n : -n], refs[-n:]

    def before(a, b):
        return a > b if backward else a < b

    me, mine = me_ref[0], me_ref[1]
    outer = jnp.zeros(outs[0].shape, f32)
    for d, piece in enumerate(far, 1):
        outer = outer + jnp.where(before(mine ^ d, mine), piece[...], 0.0)
    for d, out in enumerate(outs):
        total = outer
        for e, piece in enumerate(got):
            if e != d:
                total = total + jnp.where(before(me ^ e, me ^ d), piece[...], 0.0)
        out[...] = total


def forward_kernel(dm, scale, per, p, i, me_ref, t_ref, *rest):
    used, slots, outs = rest[:6], rest[6 : 6 + per], rest[6 + per : 9 + per]
    backs, (scr,) = rest[9 + per : 9 + 2 * per], rest[9 + 2 * per :]
    state = get_slots(me_ref, slots, scr)
    teacher = t_ref.at[head_at(me_ref, per, p)]
    put_slots(me_ref, backs, scr, forward_head(dm, scale, state, teacher, *[ref.at[i] for ref in used], *outs))


def forward_head(
    dm, scale, state, teacher, numer_ref, denom_ref, phi_ref, p1_ref, p2_ref, phi_t_ref, student_ref, g_ref, gd_ref
):
    hd = state.shape[1]
    s_pack = jnp.concatenate(split2(state), 1)
    s_pack = jnp.concatenate([s_pack, jnp.zeros((dm.lanes - dm.rows, 2 * hd), bf16)], 0)
    before = count_of(state, dm)
    back, count = 0.0, 0.0
    for rows in tiles(teacher.shape[0]):
        phi = phi_ref[rows]
        prod = dot(p1_ref[rows], s_pack) + dot(p2_ref[rows], s_pack)
        numer = numer_ref[rows] + (prod[:, :hd] + prod[:, hd:])
        weighted = phi * before
        part = denom_ref[rows]
        for c in range(0, dm.lanes, LANES):
            part = part + weighted[:, c : c + LANES]
        inv = 1.0 / jnp.sum(part, 1, keepdims=True)
        y = numer * inv
        student_ref[rows] = y.astype(bf16)
        g_numer = (y - teacher[rows].astype(f32)) * (scale * inv)
        g_denom = -jnp.sum(g_numer * y, 1, keepdims=True)
        g_ref[rows] = g_numer
        gd_ref[rows] = jnp.broadcast_to(g_denom, part.shape)
        count = count + jnp.sum(phi * g_denom, 0, keepdims=True)
        back = back + dot(phi_t_ref[:, rows], jnp.concatenate(split2(g_numer), 1))
    back = back[: dm.rows] + back[dm.rows :]
    return with_count(back[:, :hd] + back[:, hd:], count, dm)


def count_column(state, dm):
    row, lane = positions((dm.rows, dm.lanes), 0), positions((dm.rows, dm.lanes), 1)
    return jnp.sum(jnp.where(row == lane, count_of(state, dm), 0.0), 1, keepdims=True)


def backward_kernel(dm, tile, per, p0, count, me_ref, q_ref, vt_ref, *rest):
    packed, rest = rest[:4], rest[4:]
    grads, rest = rest[: 2 * count], rest[2 * count :]
    slots, (gk_ref, wgrad_ref, scr) = rest[: per * count], rest[per * count :]
    grad = 0.0
    for i in range(count):
        state = get_slots(me_ref, slots[i * per : (i + 1) * per], scr)
        at = head_at(me_ref, per, p0 + i)
        refs = [ref.at[i] for ref in packed]
        gk_ref[i], head_grad = backward_head(dm, tile, state, q_ref.at[at], vt_ref.at[at], *grads[2 * i : 2 * i + 2], *refs)
        grad = grad + head_grad
    wgrad_ref[...] = grad


def backward_head(dm, tile, state, q, vt, g_numer, g_denom, q_pack, k_pack, q_two, ext):
    w = dm.width
    s_aug = jnp.concatenate(
        [state, jnp.where(positions((1, LANES), 1) == 0, count_column(state, dm), 0.0)], 1
    )
    s1, s2 = split2(s_aug)
    count = q_pack.shape[0] // tile
    below = positions((tile, tile), 0) >= positions((tile, tile), 1)
    g_q, g_k = [], 0.0
    for i in range(count):
        rows = slice(i * tile, (i + 1) * tile)
        width = (i + 1) * tile
        t = dot(q_pack[rows], k_pack[:, :width])
        g_weight = dot(g_numer[rows].astype(bf16), vt[:, :width]) + jnp.concatenate([g_denom[rows]] * (width // LANES), 1)
        score = g_weight * t
        last = jnp.where(below, score[:, width - tile :], 0.0)
        hi, lo = split2(jnp.concatenate([score[:, : width - tile], last], 1) if i else last)
        both = dot(k_pack[: 2 * w, :width], hi, NT)
        g_q.append(both[:w] + both[w:] + dot(k_pack[:w, :width], lo, NT))
        both = dot(q_two[:, rows], hi)
        part = both[:w] + both[w:] + dot(q_two[:w, rows], lo)
        rest = count * tile - width
        g_k = g_k + (jnp.concatenate([part, jnp.zeros((w, rest), f32)], 1) if rest else part)
    first = positions((1, LANES), 1) == 0
    a1, a2 = split2(jnp.concatenate([g_numer[...], jnp.where(first, g_denom[...], 0.0)], 1))
    both = dot(jnp.concatenate([s1, s2], 0), a1, NT)
    g_phi = both[: dm.rows] + both[dm.rows :] + dot(s1, a2, NT)
    total = jnp.concatenate(g_q, 1) + feature_grad_t(ext[...], g_phi, dm)
    return g_k, dot(total.astype(bf16), q[...])


def saving_kernel(body, per, n_in, heads, me_ref, *refs):
    used, pieces, outs = refs[: n_in - 1], refs[n_in - 1 : n_in - 1 + heads], refs[n_in - 1 + heads :]
    gk_ref, wgrad_ref, dst, scr, sems = outs
    copies = [
        pltpu.make_async_copy(piece, dst.at[head_at(me_ref, per, p)], sems.at[p]) for p, piece in enumerate(pieces)
    ]
    for copy in copies:
        copy.start()
    body(me_ref, *used, gk_ref, wgrad_ref, scr)
    for copy in copies:
        copy.wait()


def key_kernel(dm, per, places, first, me_ref, k_ref, vt_ref, wk_ref, *rest):
    count = len(places)
    slots, backs = rest[: per * count], rest[per * count : (per + 1) * count]
    before, (out_ref, scr) = rest[(per + 1) * count : -2], rest[-2:]
    w = dm.width
    w_ext = rolled(wk_ref[...].astype(bf16), dm)
    grad = jnp.zeros((w, out_ref.shape[1]), f32) if first else before[0][w:]
    for at, ((p, i), gk_ref) in enumerate(zip(places, backs)):
        state = get_slots(me_ref, slots[at * per : (at + 1) * per], scr)
        h = head_at(me_ref, per, p)
        k = k_ref[h]
        g_phi = dot(state.astype(bf16), vt_ref[h]) + count_column(state, dm)
        total = gk_ref[i] + feature_grad_t(dot(w_ext, k, NT), g_phi, dm)
        grad = grad + dot(total.astype(bf16), k)
    out_ref[:w] = functools.reduce(jnp.add, [g[...] for g in before]) if first else before[0][:w]
    out_ref[w:] = grad


VMEM_LIMIT = 20 * 1024 * 1024
HBM = pl.BlockSpec(memory_space=pltpu.HBM)
VMEM = pl.BlockSpec(memory_space=pltpu.VMEM)
SMEM = pl.BlockSpec(memory_space=pltpu.SMEM)


def placed(args, specs):
    spaces = {id(HBM): pltpu.HBM, id(VMEM): pltpu.VMEM, id(SMEM): pltpu.SMEM}
    return [
        pltpu.with_memory_space_constraint(a, spaces[id(s)]) if id(s) in spaces else a
        for a, s in zip(args, specs)
    ]


def call(body, grid, args, specs, outs, out_specs, scratch, flops):
    return pl.pallas_call(
        body,
        grid=grid,
        in_specs=specs,
        out_specs=out_specs,
        out_shape=outs,
        scratch_shapes=scratch,
        compiler_params=pltpu.CompilerParams(
            dimension_semantics=("arbitrary",) * len(grid), vmem_limit_bytes=VMEM_LIMIT
        ),
        cost_estimate=pl.CostEstimate(flops=flops, bytes_accessed=0, transcendentals=0),
    )(*placed(args, specs))


def shifted(array, axis, pairs):
    return lax.ppermute(array, axis, pairs)


def crossed(array, axis, d):
    n, h = lax.axis_size(axis), lax.axis_size("head")
    return shifted(array, (axis, "head"), [(i * h + c, (i ^ d) * h + h - 1 - c) for i in range(n) for c in range(h)])


def exchange(parts, axis, cross=False):
    n = lax.axis_size(axis)
    got = []
    for d, part in enumerate(parts):
        if cross:
            got.append(crossed(part, axis, d))
        else:
            got.append(part if d == 0 else shifted(part, axis, [(i, i ^ d) for i in range(n)]))
    return got


def carried(me, parts, backward, label):
    n, m = lax.axis_size("seq"), lax.axis_size("seg")
    cross = label in CROSSED and lax.axis_size("head") > 1
    got = exchange(parts, "seq", cross)
    total = functools.reduce(jnp.add, got)
    far = exchange([total] * m, "seg")[1:]
    shape = pltpu.VMEM(parts[0].shape, f32)
    before = call(
        functools.partial(join_kernel, n, backward),
        (),
        (me, *far, *got),
        [SMEM] + [VMEM] * (n + m - 1),
        [shape] * n,
        [VMEM] * n,
        [],
        parts[0].size * n * n,
    )
    return exchange(before, "seq", cross)


def summed(array):
    array = functools.reduce(jnp.add, exchange([array] * lax.axis_size("head"), "head"))
    for axis in ("seq", "seg"):
        got = array
        for d in range(1, lax.axis_size(axis)):
            got = got + crossed(array, axis, d)
        array = got
    return array


SPLIT = (1, 2, 1)
CROSSED = ("f",)


def split_heads(heads, split):
    if heads % sum(split):
        return [(0, heads)]
    unit, at, out = heads // sum(split), 0, []
    for part in split:
        out.append((at, part * unit))
        at += part * unit
    return out


def shards(queries, keys, values, teacher, query_proj, key_proj):
    heads, tokens, hd = queries.shape
    dm = Dims(query_proj.shape[1])
    n = lax.axis_size("seq")
    assert n % heads == 0
    per = n // heads
    heads_all = heads * lax.axis_size("head")
    tokens_all = tokens * n * lax.axis_size("seg")
    scale = 1.0 / math.sqrt(heads_all * tokens_all)
    tile = min(256, tokens)
    wq, wk = query_proj.T, key_proj.T
    me = jnp.stack([lax.axis_index("seq"), lax.axis_index("seg")]).astype(jnp.int32)
    slot_shape = pltpu.VMEM((heads * dm.rows // n, hd), f32)
    grad_shape = pltpu.VMEM((dm.width, hd), f32)
    scr = [pltpu.VMEM((dm.rows, hd), f32)]

    sources = (wk, keys, values, wq)
    called = call(
        functools.partial(state_kernel, dm, n),
        (),
        (me, *sources),
        [SMEM] + [HBM] * len(sources),
        [slot_shape] * n + [pltpu.VMEM(a.shape, a.dtype) for a in sources] + [pltpu.SMEM((2,), jnp.int32)],
        [VMEM] * (n + len(sources)) + [SMEM],
        scr + [pltpu.SemaphoreType.DMA((4 + 2 * heads,))],
        4 * heads * tokens * dm.rows * hd,
    )
    states, (wk, keys, values, wq, me) = called[:n], called[n:]
    vt, queries, teacher = call(
        turn_kernel,
        (),
        (values, queries, teacher),
        [VMEM, HBM, HBM],
        [pltpu.VMEM((heads, hd, tokens), bf16)] + [pltpu.VMEM(a.shape, bf16) for a in (queries, teacher)],
        [VMEM] * 3,
        [pltpu.SemaphoreType.DMA((2,))],
        heads * tokens * hd * hd,
    )
    intra, packed, parts = [], [], split_heads(heads, SPLIT)
    for p0, count in parts:
        outs = call(
            functools.partial(intra_kernel, dm, tile, per, p0),
            (count,),
            (me, queries, keys, values, wq, wk),
            [SMEM] + [VMEM] * 5,
            [
                pltpu.VMEM((count, tokens, hd), f32),
                pltpu.VMEM((count, tokens, LANES), f32),
                pltpu.VMEM((count, tokens, LANES), bf16),
                pltpu.VMEM((count, LANES, tokens), bf16),
                pltpu.VMEM((count, 2 * dm.width, tokens), bf16),
                pltpu.VMEM((count, dm.quad, tokens), f32),
            ],
            [VMEM] * 6,
            [],
            4 * count * tokens * tokens * hd,
        )
        outs += call(
            functools.partial(feature_kernel, dm, per, p0),
            (count,),
            (me, queries, wq, outs[5]),
            [SMEM] + [VMEM] * 3,
            [
                pltpu.VMEM((count, tokens, dm.lanes), f32),
                pltpu.VMEM((count, tokens, dm.lanes), bf16),
                pltpu.VMEM((count, tokens, dm.lanes), bf16),
                pltpu.VMEM((count, 2 * dm.rows, tokens), bf16),
            ],
            [VMEM] * 4,
            [],
            4 * count * tokens * dm.lanes * hd,
        )
        intra.append(outs[:2] + outs[6:])
        packed.append(outs[2:6])
    prev = carried(me, states, False, "f")
    heads_out = {}
    for p, i, part in reversed([(p0 + i, i, part) for part, (p0, count) in enumerate(parts) for i in range(count)]):
        heads_out[p] = call(
            functools.partial(forward_kernel, dm, scale, per, p, i),
            (),
            (me, teacher, *intra[part], *prev[p * per : (p + 1) * per]),
            [SMEM] + [VMEM] * (7 + per),
            [
                pltpu.VMEM((tokens, hd), bf16),
                pltpu.VMEM((tokens, hd), f32),
                pltpu.VMEM((tokens, LANES), f32),
            ]
            + [slot_shape] * per,
            [VMEM] * (3 + per),
            scr,
            8 * tokens * dm.lanes * hd,
        )
    later = carried(me, [b for p in range(heads) for b in heads_out[p][3:]], True, "b")
    backs = []
    for part, (p0, count) in enumerate(parts):
        body = functools.partial(backward_kernel, dm, tile, per, p0, count)
        args = (me, queries, vt, *packed[part])
        for i in range(count):
            args += tuple(heads_out[p0 + i][1:3])
        args += tuple(prev[p0 * per : (p0 + count) * per])
        outs = [pltpu.VMEM((count, dm.width, tokens), f32), grad_shape]
        specs, scratch = [VMEM] * len(outs), scr
        if part == 0:
            body = functools.partial(saving_kernel, body, per, len(args), heads)
            args += tuple(heads_out[p][0] for p in range(heads))
            outs, specs = outs + [pltpu.HBM((heads, tokens, hd), bf16)], specs + [HBM]
            scratch = scr + [pltpu.SemaphoreType.DMA((heads,))]
        outs = call(
            body, (), args, [SMEM] + [VMEM] * (len(args) - 1), outs, specs, scratch, 8 * count * tokens * tokens * hd
        )
        if part == 0:
            student = outs[2]
        backs += outs[:2]
    spots = [(p0 + i, i, part) for part, (p0, count) in enumerate(parts) for i in range(count)]
    grads = backs[1::2]
    for step, group in enumerate(g for g in (spots[:1], spots[1:][-1:], spots[1:-1]) if g):
        args = (me, keys, vt, wk)
        for p, _, _ in group:
            args += tuple(later[p * per : (p + 1) * per])
        args += tuple(backs[2 * part] for _, _, part in group) + tuple(grads)
        grads = call(
            functools.partial(key_kernel, dm, per, [(p, i) for p, i, _ in group], step == 0),
            (),
            args,
            [SMEM] + [VMEM] * (len(args) - 1),
            [pltpu.VMEM((2 * dm.width, hd), f32)],
            [VMEM],
            scr,
            4 * len(group) * tokens * dm.rows * hd,
        )
    (grads,) = grads
    grads = summed(grads)
    return student, grads[: dm.width].T, grads[dm.width :].T


def solution(mesh):
    in_specs = (
        P("head", ("seg", "seq"), None),
        P("head", ("seg", "seq"), None),
        P("head", ("seg", "seq"), None),
        P("head", ("seg", "seq"), None),
        P(),
        P(),
    )
    out_specs = (P("head", ("seg", "seq"), None), P(), P())
    return jax.shard_map(shards, mesh=mesh, in_specs=in_specs, out_specs=out_specs, check_vma=False)
```
